256 devices in a mesh: groups: 4 (over x, y), gx: 64 (over z, core).
Axes of the slice: x: 2, y: 2, z: 32, core: 2. Of those that a mesh axis runs over, the one named last changes fastest.
The devices are a block of a 4x8x32 slice.
Arguments:
- velocity: float32 [2, 4096, 512], P(None, ('groups', 'gx')), parts along dimension 1, may hold values from -6 to 6
- cotangent: float32 [2, 4096, 512], P(None, ('groups', 'gx')), parts along dimension 1, may hold values from -6 to 6
- w_first: float32 [3, 3, 32, 2], replicated, may hold values from -1.5 to 1.5
- b_first: float32 [32], replicated, may hold values from -3 to 3
- w_hidden: float32 [2, 3, 3, 32, 32], replicated, may hold values from -0.375 to 0.375
- b_hidden: float32 [2, 32], replicated, may hold values from -3 to 3
- w_last: float32 [3, 3, 2, 32], replicated, may hold values from -0.375 to 0.375
Outputs:
- grad_velocity: float32 [2, 4096, 512], P(None, ('groups', 'gx')), parts along dimension 1
- grad_w_first: float32 [12, 3, 32, 2], P('groups'), parts along dimension 0
- grad_b_first: float32 [128], P('groups'), parts along dimension 0
- grad_w_hidden: float32 [8, 3, 3, 32, 32], P('groups'), parts along dimension 0
- grad_b_hidden: float32 [8, 32], P('groups'), parts along dimension 0
- grad_w_last: float32 [12, 3, 2, 32], P('groups'), parts along dimension 0
- grad_b_last: float32 [8], P('groups'), parts along dimension 0
The draws below stay inside these ranges and needn't reach their ends.
There are 4 independent parts, one for each index of `groups`. The reference program is written for one: setup_inputs(seed, part) draws one part's arguments, and reference() takes and returns one part's arrays. A program takes and returns all parts, laid end to end along the dimension named above; an argument that names none is the same for every part. Nothing has to cross between parts.
All inputs are finite; a program needn't handle non-finite values.
Results may differ from the reference program's by a relative error of at most 0.00012.
Values sent between devices are 32-bit elements; how exact they have to be, the bound alone decides.
No kernel may reach another device: no remote copies, remote signals or barrier semaphores. Data moves between devices by JAX's collectives and lax.ppermute only.
A program may use at most 128 MiB of HBM per device.

```python
import jax
import jax.numpy as jnp
from jax import lax

NY = 512
CH = 32
LAYERS = 4
ITERS = 8
NX = 1024


def steps_of(stream_key, shape, pieces, low, high):
    loudness, own = 1.0, jax.random.fold_in(stream_key, 6)
    for position, parts in pieces:
        heights = jnp.exp(jax.random.uniform(jax.random.fold_in(own, position), (parts,), jnp.float32, low / len(pieces), high / len(pieces)))
        loudness = loudness * jnp.repeat(heights, shape[position] // parts).reshape([-1 if axis == position else 1 for axis in range(len(shape))])
    return loudness


def noise(stream_key, dims, width, most, pieces=(), held_as=jnp.bfloat16):
    entries = width * jax.random.normal(stream_key, dims, jnp.float32)
    if pieces:
        entries = entries * steps_of(stream_key, dims, pieces, -0.22, 0.18)
    return jnp.clip(entries, -most, most).astype(held_as)


def setup_inputs(seed: int = 0, part: int = 0) -> dict:
    key_list = jax.random.split(jax.random.key(seed), 8)
    part_splits = jax.random.split(jax.random.fold_in(key_list[7], part), 8)
    return {
        "velocity": noise(part_splits[0], (2, NX, NY), 1.0, 6.0, ((1, 64),), jnp.float32),
        "cotangent": noise(part_splits[1], (2, NX, NY), 1.0, 6.0, ((1, 64),), jnp.float32),
        "w_first": noise(key_list[2], (3, 3, CH, 2), 18 ** -0.5, 1.5, (), jnp.float32),
        "b_first": noise(key_list[3], (CH,), 0.5, 3.0, (), jnp.float32),
        "w_hidden": noise(key_list[4], (LAYERS - 2, 3, 3, CH, CH), (9 * CH) ** -0.5, 0.375, (), jnp.float32),
        "b_hidden": noise(key_list[5], (LAYERS - 2, CH), 0.5, 3.0, (), jnp.float32),
        "w_last": noise(key_list[6], (3, 3, 2, CH), (9 * CH) ** -0.5, 0.375, (), jnp.float32),
    }


step_size = 0.25

def conv(x, w, b):
    out = b[:, None, None] + jnp.zeros((w.shape[2],) + x.shape[1:], jnp.float32)
    for p in range(3):
        for q in range(3):
            moved = jnp.roll(x, (1 - p, 1 - q), axis=(1, 2))
            out = out + jnp.einsum('ok,kxy->oxy', w[p, q], moved, precision=lax.Precision.HIGHEST)
    return out

def closure(field, params):
    w_first, b_first, w_hidden, b_hidden, w_last, b_last = params
    x = jnp.tanh(conv(field, w_first, b_first))
    for m in range(LAYERS - 2):
        x = jnp.tanh(conv(x, w_hidden[m], b_hidden[m]))
    return conv(x, w_last, b_last)

def advect(field):
    along_x = (jnp.roll(field, -1, 1) - jnp.roll(field, 1, 1)) * 0.5
    along_y = (jnp.roll(field, -1, 2) - jnp.roll(field, 1, 2)) * 0.5
    return field[0:1] * along_x + field[1:2] * along_y

def forward(field, params):
    return field + step_size * (closure(field, params) - advect(field))

def laplace(field):
    return 4.0 * field - jnp.roll(field, 1, 0) - jnp.roll(field, -1, 0) - jnp.roll(field, 1, 1) - jnp.roll(field, -1, 1)

def reference(velocity, cotangent, w_first, b_first, w_hidden, b_hidden, w_last):
    first, second = (cotangent[0], cotangent[1])
    source = -(jnp.roll(first, -1, 0) - first + (jnp.roll(second, -1, 1) - second))
    pressure = jnp.zeros_like(source)
    residual, direction = (source, source)
    norm_now = jnp.sum(residual * residual)
    for step in range(ITERS):
        image = laplace(direction)
        alpha = norm_now / jnp.sum(direction * image)
        pressure = pressure + alpha * direction
        residual = residual - alpha * image
        norm_next = jnp.sum(residual * residual)
        direction = residual + norm_next / norm_now * direction
        norm_now = norm_next
    slope = jnp.stack([pressure - jnp.roll(pressure, 1, 0), pressure - jnp.roll(pressure, 1, 1)])
    adjoint = cotangent - slope
    zero_bias = jnp.zeros((2,), jnp.float32)
    params = (w_first, b_first, w_hidden, b_hidden, w_last, zero_bias)
    unused, pull = jax.vjp(forward, velocity, params)
    grad_velocity, grads = pull(adjoint)
    factor = 1.0 / jnp.sqrt(jnp.float32(NX * NY))
    g_wf, g_bf, g_wh, g_bh, g_wl, g_bl = [item * factor for item in grads]
    return (grad_velocity, g_wf, g_bf, g_wh, g_bh, g_wl, g_bl)
```

```python
import functools

import jax
import jax.numpy as jnp
from jax import lax
from jax.experimental import pallas as pl
from jax.experimental.pallas import tpu as pltpu
from jax.sharding import Mesh
from jax.sharding import PartitionSpec as P

ITERS = 8
GX = ("gx_0", "gx_1")
GROUPS_GX = ("groups", "gx_0", "gx_1")
SPREAD_LIMIT = 3000.0
BLOCK = 6
SPAN = BLOCK + 2
F32 = jnp.float32
BF16 = jnp.bfloat16

step_size = 0.25


def from_everyone(x, axis):
    length = lax.axis_size(axis)
    return lax.all_to_all(jnp.broadcast_to(x[None], (length, *x.shape)), axis, 0, 0, tiled=True)


def shifted(value, axis, steps):
    count = lax.axis_size(axis)
    pairs = [(source, (source + steps) % count) for source in range(count)]
    return lax.ppermute(value, axis, pairs)


def turn(x, steps, axis):
    return pltpu.roll(x, steps % x.shape[axis], axis)


def halves(x):
    high = x.astype(BF16)
    return high, (x - high.astype(F32)).astype(BF16)


def starts(first, count):
    return [min(first + BLOCK * i, first + count - BLOCK) for i in range(-(-count // BLOCK))]


def fold_lanes(x):
    total = x[:, :128]
    for at in range(128, x.shape[1], 128):
        total = total + x[:, at : at + 128]
    return total


def lane_groups_summed(x):
    x = fold_lanes(x)
    x = x + turn(x, 64, 1)
    return x + turn(x, 32, 1)


def neighbours(t):
    return turn(t, 1, 0) + turn(t, -1, 0) + turn(t, 1, 1) + turn(t, -1, 1)


def basis_kernel(prev, own, later, basis, sums):
    rows = own.shape[1]
    first = jnp.concatenate([prev[0], own[0], later[0]], axis=0)
    second = jnp.concatenate([prev[1], own[1], later[1]], axis=0)
    source = -(turn(first, -1, 0) - first + (turn(second, -1, 1) - second))
    line = lax.broadcasted_iota(jnp.int32, (2 * ITERS, 128), 0)
    lane = lax.broadcasted_iota(jnp.int32, (2 * ITERS, 128), 1)
    squares, crosses = [], []

    def product(a, b):
        return fold_lanes(jnp.sum(a[rows : 2 * rows] * b[rows : 2 * rows], axis=0, keepdims=True))

    before, now = None, source
    for k in range(ITERS):
        basis[k] = now[rows - 8 : 2 * rows + 8]
        if k == 0:
            after = -0.25 * neighbours(now)
        else:
            after = -0.5 * neighbours(now) - before
        squares.append(product(now, now))
        crosses.append(product(now, after))
        before, now = now, after
    stacked = jnp.concatenate(squares + crosses, axis=0)
    column = jnp.sum(stacked, axis=1, keepdims=True)
    row = jnp.sum(jnp.where(line == lane, column, 0.0), axis=0, keepdims=True)
    sums[...] = jnp.broadcast_to(row, sums.shape)


def quadratic(a, b, mu):
    total = None
    for i, left in enumerate(a):
        inner = None
        for j, right in enumerate(b):
            term = right * mu[i][j]
            inner = term if inner is None else inner + term
        total = left * inner if total is None else total + left * inner
    return total


def spread(a):
    total = jnp.abs(a[0])
    for item in a[1:]:
        total = total + jnp.abs(item)
    return total


def image_of(c):
    out = [4.0 * item for item in c] + [jnp.zeros_like(c[0])]
    out[1] = out[1] + 4.0 * c[0]
    for k in range(1, len(c)):
        out[k + 1] = out[k + 1] + 2.0 * c[k]
        out[k - 1] = out[k - 1] + 2.0 * c[k]
    return out


def combined(factor, a, b):
    out = []
    for k in range(max(len(a), len(b))):
        if k >= len(a):
            out.append(b[k])
        elif k >= len(b):
            out.append(factor * a[k])
        else:
            out.append(b[k] + factor * a[k])
    return out


def pressure_kernel(gathered, basis, pressure, unsafe):
    total = jnp.sum(gathered[...], axis=0, keepdims=True)
    lane = lax.broadcasted_iota(jnp.int32, (1, 128), 1)
    items = [
        jnp.broadcast_to(jnp.sum(jnp.where(lane == k, total, 0.0), axis=1, keepdims=True), (1, 128))
        for k in range(2 * ITERS)
    ]
    moments = [items[0], items[ITERS]]
    for k in range(1, ITERS):
        moments.append(2.0 * items[k] - items[0])
        moments.append(2.0 * items[ITERS + k] - items[ITERS])
    mu = [
        [0.5 * (moments[i + j] + moments[abs(i - j)]) for j in range(min(ITERS + 1, 2 * ITERS - i))]
        for i in range(ITERS)
    ]
    one = jnp.ones((1, 128), F32)
    residual, direction, answer = [one], [one], [jnp.zeros((1, 128), F32)]
    norm_now = items[0]
    safe = norm_now > 0.0
    for step in range(ITERS):
        image = image_of(direction)
        product = quadratic(direction, image, mu)
        bound = spread(direction) * spread(image) * items[0]
        safe = safe & (product > 0.0) & (bound < SPREAD_LIMIT * product)
        alpha = norm_now / product
        answer = combined(alpha, direction, answer)
        if step + 1 < ITERS:
            residual = combined(-alpha, image, residual)
            norm_next = quadratic(residual, residual, mu)
            size = spread(residual)
            safe = safe & (norm_next > 0.0) & (size * size * items[0] < SPREAD_LIMIT * norm_next)
            direction = combined(norm_next / norm_now, direction, residual)
            norm_now = norm_next
    wide = basis.shape[2] // 128
    lam = None
    for k in range(ITERS):
        term = jnp.concatenate([answer[k]] * wide, axis=1) * basis[k]
        lam = term if lam is None else lam + term
    pressure[...] = lam
    unsafe[...] = jnp.where(safe, 0, 1).astype(jnp.int32)


def laplace(field):
    above = shifted(field[-1:], GX, 1)
    below = shifted(field[:1], GX, -1)
    up = jnp.concatenate([above, field[:-1]], axis=0)
    down = jnp.concatenate([field[1:], below], axis=0)
    return 4.0 * field - up - down - jnp.roll(field, 1, 1) - jnp.roll(field, -1, 1)


def sum_of(a, b):
    local = jnp.broadcast_to(jnp.sum(a * b), (1, 128))
    return jnp.sum(from_everyone(local, GX)[:, 0, 0])


def stepwise_pressure(cotangent, later):
    first, second = cotangent[0], cotangent[1]
    below = jnp.concatenate([first[1:], later[0, :1]], axis=0)
    source = -(below - first + (jnp.roll(second, -1, 1) - second))

    def iterate(_, carry):
        pressure, residual, direction, norm_now = carry
        image = laplace(direction)
        alpha = norm_now / sum_of(direction, image)
        pressure = pressure + alpha * direction
        residual = residual - alpha * image
        norm_next = sum_of(residual, residual)
        direction = residual + norm_next / norm_now * direction
        return pressure, residual, direction, norm_next

    start = (jnp.zeros_like(source), source, source, sum_of(source, source))
    pressure = lax.fori_loop(0, ITERS, iterate, start)[0]
    above = shifted(pressure[-8:], GX, 1)
    under = shifted(pressure[:8], GX, -1)
    return jnp.concatenate([above, pressure, under], axis=0)


def banded(taps):
    rows = jnp.concatenate([taps] + [turn(taps, 32 * r, 1) for r in range(1, BLOCK)], axis=0)
    high, low = halves(rows)
    return jnp.concatenate([high, high, low], axis=1)


def banded_narrow(taps):
    rows = jnp.concatenate([taps] + [turn(taps, r, 1) for r in range(1, BLOCK)], axis=0)
    high = rows.astype(BF16).astype(F32)
    low = rows - high
    return (high + turn(high, 16, 1) + turn(low, 32, 1)).astype(BF16)[:, :48]


def banded_out(taps, rows):
    width = (rows + 2) * 32
    padded = -(-width // 128)
    lane = lax.broadcasted_iota(jnp.int32, (rows, padded * 128), 1) // 32
    row = lax.broadcasted_iota(jnp.int32, (rows, padded * 128), 0)
    pieces = []
    for j in range(6):
        piece = jnp.zeros((rows, padded * 128), F32)
        for p in range(3):
            line = jnp.concatenate([taps[p][j : j + 1]] * padded, axis=1)
            piece = piece + jnp.where(lane == row + p, line, 0.0)
        pieces.append(piece)
    return halves(jnp.concatenate(pieces, axis=0))


def side_sum(y):
    n = y.shape[1] // 3
    return turn(y[:, :n], 1, 2) + y[:, n : 2 * n] + turn(y[:, 2 * n :], -1, 2)


def wide_conv(weights, high, low):
    x = jnp.concatenate([high, low, high], axis=0)
    y = jnp.dot(weights, x, preferred_element_type=F32)
    return side_sum(y.reshape(BLOCK, 96, y.shape[1]))


def narrow_conv(weights, pair):
    high, low = halves(jnp.concatenate(pair, axis=0))
    x = jnp.concatenate([high, low, high], axis=0)
    y = jnp.dot(weights, x, preferred_element_type=F32)
    return side_sum(y.reshape(BLOCK, 96, y.shape[1]))


def put(refs, at, value):
    high, low = halves(value.reshape(value.shape[0] * 32, value.shape[2]))
    span = pl.ds(at * 32, value.shape[0] * 32)
    refs[0][span, :] = high
    refs[1][span, :] = low


def take(refs, at, rows):
    span = pl.ds(at * 32, rows * 32)
    return refs[0][span, :], refs[1][span, :]


def forward_kernel(
    prev, own, later, narrow, wide, bias, a0h, a0l, a1h, a1l, a2h, a2l, weights0, weights1, weights2
):
    rows, width = own.shape[1], own.shape[2]
    v = [jnp.concatenate([prev[c, rows - 8 :], own[c], later[c, :8]], axis=0) for c in range(2)]
    weights0[...] = banded_narrow(narrow[...])
    weights1[...] = banded(wide[0])
    weights2[...] = banded(wide[1])
    shift = [jnp.concatenate([bias[m]] * (width // 128), axis=1) for m in range(3)]
    for s in starts(-5, rows + 10):
        pair = [v[c][s + 7 : s + 7 + SPAN] for c in range(2)]
        put((a0h, a0l), s + 5, jnp.tanh(narrow_conv(weights0[...], pair) + shift[0]))
    for s in starts(-4, rows + 8):
        x = take((a0h, a0l), s + 4, SPAN)
        put((a1h, a1l), s + 4, jnp.tanh(wide_conv(weights1[...], *x) + shift[1]))
    for s in starts(-3, rows + 6):
        x = take((a1h, a1l), s + 3, SPAN)
        put((a2h, a2l), s + 3, jnp.tanh(wide_conv(weights2[...], *x) + shift[2]))


def dot_nt(a, b):
    return lax.dot_general(a, b, (((1,), (1,)), ((), ())), preferred_element_type=F32)


def sided(e, axis):
    return jnp.concatenate([turn(e, -1, e.ndim - 1), e, turn(e, 1, e.ndim - 1)], axis=axis)


def wide_terms(err, err_at, act, act_at, rows):
    total = None
    lines = -(-rows // BLOCK)
    for i in range(lines):
        s = min(BLOCK * i, rows - BLOCK)
        e = err[pl.ds((err_at + s) * 32, BLOCK * 32), :].reshape(BLOCK, 32, -1)
        spent = BLOCK * i - s
        if spent:
            e = jnp.concatenate([jnp.zeros_like(e[:spent]), e[spent:]], axis=0)
        high, low = halves(sided(e, 1).reshape(BLOCK * 96, -1))
        ah, al = take(act, act_at + s - 1, SPAN)
        term = dot_nt(
            jnp.concatenate([high, high, low], axis=1), jnp.concatenate([ah, al, ah], axis=1)
        )
        total = term if total is None else total + term
    total = total.reshape(BLOCK, 96, SPAN * 32)
    out = None
    for r in range(BLOCK):
        piece = turn(total[r], -32 * r, 1)[:, :128]
        out = piece if out is None else out + piece
    return out


def eight_rows(x):
    missing = 8 - x.shape[0]
    if not missing:
        return x
    return jnp.concatenate([x, jnp.zeros((missing, x.shape[1]), x.dtype)], axis=0)


def bias_line(err, err_at, rows):
    e = err[pl.ds(err_at * 32, rows * 32), :].reshape(rows, 32, -1)
    column = jnp.sum(fold_lanes(jnp.sum(e, axis=0)), axis=1, keepdims=True)
    line = lax.broadcasted_iota(jnp.int32, (32, 128), 0)
    lane = lax.broadcasted_iota(jnp.int32, (32, 128), 1)
    return eight_rows(jnp.sum(jnp.where(lane == line + 96, column, 0.0), axis=0, keepdims=True))


def backward_kernel(
    factor,
    pressure,
    cprev,
    cown,
    clater,
    vprev,
    vown,
    vlater,
    a0h,
    a0l,
    a1h,
    a1l,
    a2h,
    a2l,
    narrow,
    wide,
    out_taps,
    grad_velocity,
    terms,
    e2,
    e1,
    e0,
    eh,
    el,
    weights,
    weights_narrow,
):
    rows, width = vown.shape[1], vown.shape[2]
    a0, a1, a2, split = (a0h, a0l), (a1h, a1l), (a2h, a2l), (eh, el)

    def extended(prev, own, later, c):
        return jnp.concatenate([prev[c, rows - 8 :], own[c], later[c, :8]], axis=0)

    lam = pressure[...]
    adjoint = [
        extended(cprev, cown, clater, 0) - (lam - turn(lam, 1, 0)),
        extended(cprev, cown, clater, 1) - (lam - turn(lam, 1, 1)),
    ]
    v = [extended(vprev, vown, vlater, c) for c in range(2)]
    e3 = [step_size * item for item in adjoint]

    def slope_of(act, at):
        high, low = take(act, at, BLOCK)
        a = high.astype(F32) + low.astype(F32)
        return (1.0 - a * a).reshape(BLOCK, 32, width)

    def keep(ref, at, value):
        put(split, at, value)
        ref[pl.ds(at * 32, BLOCK * 32), :] = value.reshape(BLOCK * 32, width)

    weights_narrow[...] = banded_narrow(narrow[...])
    for s in starts(-3, rows + 6):
        pair = [e3[c][s + 7 : s + 7 + SPAN] for c in range(2)]
        keep(e2, s + 3, narrow_conv(weights_narrow[...], pair) * slope_of(a2, s + 3))
    weights[...] = banded(wide[1])
    for s in starts(-2, rows + 4):
        x = take(split, s + 2, SPAN)
        e1[pl.ds((s + 2) * 32, BLOCK * 32), :] = (
            wide_conv(weights[...], *x) * slope_of(a1, s + 4)
        ).reshape(BLOCK * 32, width)
    split_rows = (rows + 4) * 32
    high, low = halves(e1[...])
    eh[0:split_rows, :] = high
    el[0:split_rows, :] = low
    weights[...] = banded(wide[0])
    for s in starts(-1, rows + 2):
        x = take(split, s + 1, SPAN)
        e0[pl.ds((s + 1) * 32, BLOCK * 32), :] = (
            wide_conv(weights[...], *x) * slope_of(a0, s + 5)
        ).reshape(BLOCK * 32, width)

    own = slice(8, 8 + rows)
    wh, wl = banded_out(out_taps, rows)
    high, low = halves(e0[...])
    cells = (rows + 2) * 32
    wh, wl = wh[:, :cells], wl[:, :cells]
    y = (
        jnp.dot(wh, high, preferred_element_type=F32)
        + jnp.dot(wh, low, preferred_element_type=F32)
        + jnp.dot(wl, high, preferred_element_type=F32)
    )
    through = []
    for c in range(2):
        parts = [y[(2 * q + c) * rows : (2 * q + c + 1) * rows] for q in range(3)]
        through.append(turn(parts[0], 1, 1) + parts[1] + turn(parts[2], -1, 1))

    cross = []
    for k in range(2):
        flux = v[0] * adjoint[k]
        side = v[1][own] * adjoint[k][own]
        cross.append(
            ((turn(flux, -1, 0) - turn(flux, 1, 0)) * 0.5)[own]
            + (turn(side, -1, 1) - turn(side, 1, 1)) * 0.5
        )
    along_x = [((turn(f, -1, 0) - turn(f, 1, 0)) * 0.5)[own] for f in v]
    along_y = [(turn(f[own], -1, 1) - turn(f[own], 1, 1)) * 0.5 for f in v]
    direct = [
        adjoint[0][own] * along_x[0] + adjoint[1][own] * along_x[1],
        adjoint[0][own] * along_y[0] + adjoint[1][own] * along_y[1],
    ]
    for k in range(2):
        grad_velocity[k] = adjoint[k][own] - step_size * (direct[k] - cross[k]) + through[k]

    scale = factor[0, 0]
    middle1 = wide_terms(e2, 3, a1, 4, rows)
    middle0 = wide_terms(e1, 2, a0, 5, rows)

    outer = jnp.concatenate([sided(e3[c][own], 0) for c in range(2)], axis=0)
    lh, ll = halves(outer)
    ah, al = take(a2, 2, rows + 4)
    last = dot_nt(lh, ah) + dot_nt(lh, al) + dot_nt(ll, ah)
    last = last.reshape(6, rows, (rows + 4) * 32)
    group = lax.broadcasted_iota(jnp.int32, (rows, (rows + 4) * 32), 1) // 32
    line = lax.broadcasted_iota(jnp.int32, (rows, (rows + 4) * 32), 0)
    spare = []
    for p in range(3):
        picked = jnp.sum(jnp.where((group == line + p)[None], last, 0.0), axis=1)
        spare.append(eight_rows(lane_groups_summed(picked)))

    inner = jnp.concatenate(
        [jnp.concatenate([turn(f, 1, 1), f, turn(f, -1, 1)], axis=0) for f in v], axis=0
    )
    lh, ll = halves(inner)
    eh0, el0 = high[32 : 32 + rows * 32], low[32 : 32 + rows * 32]
    begin = dot_nt(lh, eh0) + dot_nt(lh, el0) + dot_nt(ll, eh0)
    tall = rows + 16
    begin = begin.reshape(6, tall, rows * 32)
    group = lax.broadcasted_iota(jnp.int32, (tall, rows * 32), 1) // 32
    line = lax.broadcasted_iota(jnp.int32, (tall, rows * 32), 0)
    for p in range(3):
        picked = jnp.sum(jnp.where((line == group + p + 7)[None], begin, 0.0), axis=1)
        spare.append(eight_rows(lane_groups_summed(picked)))

    spare.append(bias_line(e2, 3, rows))
    spare.append(bias_line(e1, 2, rows))
    spare.append(bias_line(e0, 1, rows))
    lane = lax.broadcasted_iota(jnp.int32, (1, 128), 1)
    ends = jnp.zeros((1, 128), F32)
    for c in range(2):
        end = jnp.sum(jnp.sum(e3[c][own], axis=0, keepdims=True), axis=1, keepdims=True)
        ends = ends + jnp.where(lane == 96 + c, end, 0.0)
    spare.append(eight_rows(ends))
    spare.append(jnp.zeros((96 - 8 * len(spare), 128), F32))
    spare = jnp.concatenate(spare, axis=0)
    kept = lax.broadcasted_iota(jnp.int32, (96, 128), 1) < 96
    terms[0:96, :] = jnp.where(kept, middle1, spare) * scale
    terms[96:192, :] = jnp.where(kept, middle0, 0.0) * scale


def total_of(packed):
    far, near = lax.axis_size("gx_0"), lax.axis_size("gx_1")
    lines, lanes = packed.shape
    half = lax.all_to_all(packed.reshape(near, lines // near, lanes), "gx_1", 0, 0, tiled=True)
    half = half.sum(axis=0)
    part = lax.all_to_all(half.reshape(far, -1, lanes), "gx_0", 0, 0, tiled=True).sum(axis=0)
    half = from_everyone(part, "gx_0").reshape(lines // near, lanes)
    return from_everyone(half, "gx_1").reshape(lines, lanes)


def forward_taps(w):
    out, into = w.shape[2], w.shape[3]
    return jnp.transpose(w, (1, 2, 0, 3)).reshape(3 * out, 3 * into)


def backward_taps(w):
    out, into = w.shape[2], w.shape[3]
    return jnp.transpose(w[::-1, ::-1], (1, 3, 0, 2)).reshape(3 * into, 3 * out)


def narrow_taps(w):
    t = jnp.transpose(w, (1, 2, 3, 0)).reshape(3 * w.shape[2], 2, 3)
    t = jnp.pad(t, ((0, 0), (0, 0), (0, 5))).reshape(-1, 16)
    return jnp.pad(t, ((0, 0), (0, 112)))


def out_taps_of(w):
    t = jnp.pad(w.reshape(3, 6, w.shape[3]), ((0, 0), (0, 2), (0, 0)))
    return jnp.concatenate([t] * 4, axis=2)


def flipped(w):
    return jnp.swapaxes(w[::-1, ::-1], 2, 3)


def shape_of(*dims, dtype=F32):
    return jax.ShapeDtypeStruct(dims, dtype)


def call(kernel, out_shape, scratch=(), **extra):
    return pl.pallas_call(
        kernel,
        out_shape=out_shape,
        scratch_shapes=list(scratch),
        compiler_params=pltpu.CompilerParams(vmem_limit_bytes=60 * 1024 * 1024),
        **extra,
    )


def body(velocity, cotangent, w_first, b_first, w_hidden, b_hidden, w_last):
    rows, width = velocity.shape[1], velocity.shape[2]
    members = lax.axis_size(GX)
    cprev, clater = shifted(cotangent, GX, 1), shifted(cotangent, GX, -1)
    vprev, vlater = shifted(velocity, GX, 1), shifted(velocity, GX, -1)

    wide_pad = ((0, 0), (0, 256 - 96))
    wide = jnp.stack([jnp.pad(forward_taps(w_hidden[m]), wide_pad) for m in range(2)])
    wide_back = jnp.stack([jnp.pad(backward_taps(w_hidden[m]), wide_pad) for m in range(2)])
    narrow = narrow_taps(w_first)
    narrow_back = narrow_taps(flipped(w_last))
    out_taps = out_taps_of(flipped(w_first))
    biases = jnp.stack([b_first, b_hidden[0], b_hidden[1]])
    biases = jnp.broadcast_to(biases[:, :, None], (3, biases.shape[1], 128))

    basis, sums = call(
        basis_kernel, (shape_of(ITERS, rows + 16, width), shape_of(members, 128))
    )(cprev, cotangent, clater)
    gathered = lax.all_to_all(sums.reshape(members, 1, 128), GX, 0, 0, tiled=True)

    heights = (rows + 10, rows + 8, rows + 6)
    held = [shape_of(h * 32, width, dtype=BF16) for h in heights for _ in range(2)]
    actives = call(
        forward_kernel,
        tuple(held),
        [
            pltpu.VMEM((96 * BLOCK, 48), BF16),
            pltpu.VMEM((96 * BLOCK, 3 * SPAN * 32), BF16),
            pltpu.VMEM((96 * BLOCK, 3 * SPAN * 32), BF16),
        ],
    )(vprev, velocity, vlater, narrow, wide, biases)

    quick, unsafe = call(
        pressure_kernel, (shape_of(rows + 16, width), shape_of(1, 128, dtype=jnp.int32))
    )(gathered.reshape(members, 128), basis)
    pressure = lax.cond(
        unsafe[0, 0] != 0,
        lambda c, l, _: stepwise_pressure(c, l),
        lambda c, l, q: q,
        cotangent,
        clater,
        quick,
    )

    factor = 1.0 / jnp.sqrt(jnp.float32(members * rows * width))
    whole = pl.BlockSpec(memory_space=pltpu.VMEM)
    grad_velocity, terms = call(
        backward_kernel,
        (shape_of(2, rows, width), shape_of(192, 128)),
        [
            pltpu.VMEM(((rows + 6) * 32, width), F32),
            pltpu.VMEM(((rows + 4) * 32, width), F32),
            pltpu.VMEM(((rows + 2) * 32, width), F32),
            pltpu.VMEM(((rows + 6) * 32, width), BF16),
            pltpu.VMEM(((rows + 6) * 32, width), BF16),
            pltpu.VMEM((96 * BLOCK, 3 * SPAN * 32), BF16),
            pltpu.VMEM((96 * BLOCK, 48), BF16),
        ],
        in_specs=[pl.BlockSpec(memory_space=pltpu.SMEM)] + [whole] * 16,
    )(
        factor.reshape(1, 1),
        pressure,
        cprev,
        cotangent,
        clater,
        vprev,
        velocity,
        vlater,
        *actives,
        narrow_back,
        wide_back,
        out_taps,
    )
    total = total_of(terms)

    def square(block):
        return jnp.transpose(block.reshape(3, 32, 3, 32), (2, 0, 1, 3))

    spare = total[:96, 96:]
    grad_hidden = jnp.stack([square(total[96:, :96]), square(total[:96, :96])])
    last = spare[:24].reshape(3, 8, 32)[:, :6]
    grad_last = jnp.swapaxes(last.reshape(3, 2, 3, 32), 1, 2)
    begin = spare[24:48].reshape(3, 8, 32)[:, :6]
    grad_first = jnp.transpose(begin.reshape(3, 2, 3, 32), (0, 2, 3, 1))
    return (
        grad_velocity,
        grad_first,
        spare[64],
        grad_hidden,
        jnp.stack([spare[56], spare[48]]),
        grad_last,
        spare[72, :2],
    )


def solution(mesh):
    cores = 2
    finer = Mesh(
        mesh.devices.reshape(mesh.shape["groups"], mesh.shape["gx"] // cores, cores), GROUPS_GX
    )
    placed = (P(None, GROUPS_GX, None), P(None, GROUPS_GX, None), P(), P(), P(), P(), P())
    return jax.shard_map(
        body,
        mesh=finer,
        in_specs=placed,
        out_specs=(
            P(None, GROUPS_GX, None),
            P("groups", None, None, None),
            P("groups"),
            P("groups", None, None, None, None),
            P("groups", None),
            P("groups", None, None, None),
            P("groups"),
        ),
        check_vma=False,
    )
```

```python
import functools

import jax
import jax.numpy as jnp
from jax import lax
from jax.experimental import pallas as pl
from jax.experimental.pallas import tpu as pltpu
from jax.sharding import Mesh
from jax.sharding import PartitionSpec as P

ITERS = 8
FAR, NEAR, CORE = "gx_far", "gx_near", "gx_core"
GX = (FAR, NEAR, CORE)
GROUPS_GX = ("groups", FAR, NEAR, CORE)
SPREAD_LIMIT = 3000.0
BLOCK = 6
SPAN = BLOCK + 2
F32 = jnp.float32
BF16 = jnp.bfloat16

step_size = 0.25


def from_everyone(x, axis):
    length = lax.axis_size(axis)
    return lax.all_to_all(jnp.broadcast_to(x[None], (length, *x.shape)), axis, 0, 0, tiled=True)


def shifted(value, axis, steps):
    count = lax.axis_size(axis)
    pairs = [(source, (source + steps) % count) for source in range(count)]
    return lax.ppermute(value, axis, pairs)


def turn(x, steps, axis):
    return pltpu.roll(x, steps % x.shape[axis], axis)


def halves(x):
    high = x.astype(BF16)
    return high, (x - high.astype(F32)).astype(BF16)


def starts(first, count):
    return [min(first + BLOCK * i, first + count - BLOCK) for i in range(-(-count // BLOCK))]


def fold_lanes(x):
    total = x[:, :128]
    for at in range(128, x.shape[1], 128):
        total = total + x[:, at : at + 128]
    return total


def lane_groups_summed(x):
    x = fold_lanes(x)
    x = x + turn(x, 64, 1)
    return x + turn(x, 32, 1)


def neighbours(t):
    return turn(t, 1, 0) + turn(t, -1, 0) + turn(t, 1, 1) + turn(t, -1, 1)


def basis_kernel(prev, own, later, basis, sums):
    rows = own.shape[1]
    first = jnp.concatenate([prev[0], own[0], later[0]], axis=0)
    second = jnp.concatenate([prev[1], own[1], later[1]], axis=0)
    source = -(turn(first, -1, 0) - first + (turn(second, -1, 1) - second))
    line = lax.broadcasted_iota(jnp.int32, (2 * ITERS, 128), 0)
    lane = lax.broadcasted_iota(jnp.int32, (2 * ITERS, 128), 1)
    squares, crosses = [], []

    def product(a, b):
        return fold_lanes(jnp.sum(a[rows : 2 * rows] * b[rows : 2 * rows], axis=0, keepdims=True))

    before, now = None, source
    for k in range(ITERS):
        basis[k] = now[rows - 8 : 2 * rows + 8]
        if k == 0:
            after = -0.25 * neighbours(now)
        else:
            after = -0.5 * neighbours(now) - before
        squares.append(product(now, now))
        crosses.append(product(now, after))
        before, now = now, after
    stacked = jnp.concatenate(squares + crosses, axis=0)
    column = jnp.sum(stacked, axis=1, keepdims=True)
    row = jnp.sum(jnp.where(line == lane, column, 0.0), axis=0, keepdims=True)
    sums[...] = jnp.broadcast_to(row, sums.shape)


def quadratic(a, b, mu):
    total = None
    for i, left in enumerate(a):
        inner = None
        for j, right in enumerate(b):
            term = right * mu[i][j]
            inner = term if inner is None else inner + term
        total = left * inner if total is None else total + left * inner
    return total


def spread(a):
    total = jnp.abs(a[0])
    for item in a[1:]:
        total = total + jnp.abs(item)
    return total


def image_of(c):
    out = [4.0 * item for item in c] + [jnp.zeros_like(c[0])]
    out[1] = out[1] + 4.0 * c[0]
    for k in range(1, len(c)):
        out[k + 1] = out[k + 1] + 2.0 * c[k]
        out[k - 1] = out[k - 1] + 2.0 * c[k]
    return out


def combined(factor, a, b):
    out = []
    for k in range(max(len(a), len(b))):
        if k >= len(a):
            out.append(b[k])
        elif k >= len(b):
            out.append(factor * a[k])
        else:
            out.append(b[k] + factor * a[k])
    return out


def pressure_kernel(gathered, basis, pressure, unsafe):
    total = jnp.sum(gathered[...], axis=0, keepdims=True)
    lane = lax.broadcasted_iota(jnp.int32, (1, 128), 1)
    items = [
        jnp.broadcast_to(jnp.sum(jnp.where(lane == k, total, 0.0), axis=1, keepdims=True), (1, 128))
        for k in range(2 * ITERS)
    ]
    moments = [items[0], items[ITERS]]
    for k in range(1, ITERS):
        moments.append(2.0 * items[k] - items[0])
        moments.append(2.0 * items[ITERS + k] - items[ITERS])
    mu = [
        [0.5 * (moments[i + j] + moments[abs(i - j)]) for j in range(min(ITERS + 1, 2 * ITERS - i))]
        for i in range(ITERS)
    ]
    one = jnp.ones((1, 128), F32)
    residual, direction, answer = [one], [one], [jnp.zeros((1, 128), F32)]
    norm_now = items[0]
    safe = norm_now > 0.0
    for step in range(ITERS):
        image = image_of(direction)
        product = quadratic(direction, image, mu)
        bound = spread(direction) * spread(image) * items[0]
        safe = safe & (product > 0.0) & (bound < SPREAD_LIMIT * product)
        alpha = norm_now / product
        answer = combined(alpha, direction, answer)
        if step + 1 < ITERS:
            residual = combined(-alpha, image, residual)
            norm_next = quadratic(residual, residual, mu)
            size = spread(residual)
            safe = safe & (norm_next > 0.0) & (size * size * items[0] < SPREAD_LIMIT * norm_next)
            direction = combined(norm_next / norm_now, direction, residual)
            norm_now = norm_next
    wide = basis.shape[2] // 128
    lam = None
    for k in range(ITERS):
        term = jnp.concatenate([answer[k]] * wide, axis=1) * basis[k]
        lam = term if lam is None else lam + term
    pressure[...] = lam
    unsafe[...] = jnp.where(safe, 0, 1).astype(jnp.int32)


def laplace(field):
    above = shifted(field[-1:], GX, 1)
    below = shifted(field[:1], GX, -1)
    up = jnp.concatenate([above, field[:-1]], axis=0)
    down = jnp.concatenate([field[1:], below], axis=0)
    return 4.0 * field - up - down - jnp.roll(field, 1, 1) - jnp.roll(field, -1, 1)


def sum_of(a, b):
    local = jnp.broadcast_to(jnp.sum(a * b), (1, 128))
    return jnp.sum(from_everyone(local, GX)[:, 0, 0])


def stepwise_pressure(cotangent, later):
    first, second = cotangent[0], cotangent[1]
    below = jnp.concatenate([first[1:], later[0, :1]], axis=0)
    source = -(below - first + (jnp.roll(second, -1, 1) - second))

    def iterate(_, carry):
        pressure, residual, direction, norm_now = carry
        image = laplace(direction)
        alpha = norm_now / sum_of(direction, image)
        pressure = pressure + alpha * direction
        residual = residual - alpha * image
        norm_next = sum_of(residual, residual)
        direction = residual + norm_next / norm_now * direction
        return pressure, residual, direction, norm_next

    start = (jnp.zeros_like(source), source, source, sum_of(source, source))
    pressure = lax.fori_loop(0, ITERS, iterate, start)[0]
    above = shifted(pressure[-8:], GX, 1)
    under = shifted(pressure[:8], GX, -1)
    return jnp.concatenate([above, pressure, under], axis=0)


def banded(taps):
    rows = jnp.concatenate([taps] + [turn(taps, 32 * r, 1) for r in range(1, BLOCK)], axis=0)
    high, low = halves(rows)
    return jnp.concatenate([high, high, low], axis=1)


def banded_narrow(taps):
    rows = jnp.concatenate([taps] + [turn(taps, r, 1) for r in range(1, BLOCK)], axis=0)
    high = rows.astype(BF16).astype(F32)
    low = rows - high
    return (high + turn(high, 16, 1) + turn(low, 32, 1)).astype(BF16)[:, :48]


def banded_out(taps, rows):
    width = (rows + 2) * 32
    padded = -(-width // 128)
    lane = lax.broadcasted_iota(jnp.int32, (rows, padded * 128), 1) // 32
    row = lax.broadcasted_iota(jnp.int32, (rows, padded * 128), 0)
    pieces = []
    for j in range(6):
        piece = jnp.zeros((rows, padded * 128), F32)
        for p in range(3):
            line = jnp.concatenate([taps[p][j : j + 1]] * padded, axis=1)
            piece = piece + jnp.where(lane == row + p, line, 0.0)
        pieces.append(piece)
    return halves(jnp.concatenate(pieces, axis=0))


def side_sum(y):
    n = y.shape[1] // 3
    return turn(y[:, :n], 1, 2) + y[:, n : 2 * n] + turn(y[:, 2 * n :], -1, 2)


def wide_conv(weights, high, low):
    x = jnp.concatenate([high, low, high], axis=0)
    y = jnp.dot(weights, x, preferred_element_type=F32)
    return side_sum(y.reshape(BLOCK, 96, y.shape[1]))


def narrow_conv(weights, pair):
    high, low = halves(jnp.concatenate(pair, axis=0))
    x = jnp.concatenate([high, low, high], axis=0)
    y = jnp.dot(weights, x, preferred_element_type=F32)
    return side_sum(y.reshape(BLOCK, 96, y.shape[1]))


def put(refs, at, value):
    high, low = halves(value.reshape(value.shape[0] * 32, value.shape[2]))
    span = pl.ds(at * 32, value.shape[0] * 32)
    refs[0][span, :] = high
    refs[1][span, :] = low


def take(refs, at, rows):
    span = pl.ds(at * 32, rows * 32)
    return refs[0][span, :], refs[1][span, :]


def forward_kernel(
    prev, own, later, narrow, wide, bias, a0h, a0l, a1h, a1l, a2h, a2l, weights0, weights1, weights2
):
    rows, width = own.shape[1], own.shape[2]
    v = [jnp.concatenate([prev[c, rows - 8 :], own[c], later[c, :8]], axis=0) for c in range(2)]
    weights0[...] = banded_narrow(narrow[...])
    weights1[...] = banded(wide[0])
    weights2[...] = banded(wide[1])
    shift = [jnp.concatenate([bias[m]] * (width // 128), axis=1) for m in range(3)]
    for s in starts(-5, rows + 10):
        pair = [v[c][s + 7 : s + 7 + SPAN] for c in range(2)]
        put((a0h, a0l), s + 5, jnp.tanh(narrow_conv(weights0[...], pair) + shift[0]))
    for s in starts(-4, rows + 8):
        x = take((a0h, a0l), s + 4, SPAN)
        put((a1h, a1l), s + 4, jnp.tanh(wide_conv(weights1[...], *x) + shift[1]))
    for s in starts(-3, rows + 6):
        x = take((a1h, a1l), s + 3, SPAN)
        put((a2h, a2l), s + 3, jnp.tanh(wide_conv(weights2[...], *x) + shift[2]))


def dot_nt(a, b):
    return lax.dot_general(a, b, (((1,), (1,)), ((), ())), preferred_element_type=F32)


def sided(e, axis):
    return jnp.concatenate([turn(e, -1, e.ndim - 1), e, turn(e, 1, e.ndim - 1)], axis=axis)


def wide_terms(err, err_at, act, act_at, rows):
    total = None
    lines = -(-rows // BLOCK)
    for i in range(lines):
        s = min(BLOCK * i, rows - BLOCK)
        e = err[pl.ds((err_at + s) * 32, BLOCK * 32), :].reshape(BLOCK, 32, -1)
        spent = BLOCK * i - s
        if spent:
            e = jnp.concatenate([jnp.zeros_like(e[:spent]), e[spent:]], axis=0)
        high, low = halves(sided(e, 1).reshape(BLOCK * 96, -1))
        ah, al = take(act, act_at + s - 1, SPAN)
        term = dot_nt(
            jnp.concatenate([high, high, low], axis=1), jnp.concatenate([ah, al, ah], axis=1)
        )
        total = term if total is None else total + term
    total = total.reshape(BLOCK, 96, SPAN * 32)
    out = None
    for r in range(BLOCK):
        piece = turn(total[r], -32 * r, 1)[:, :128]
        out = piece if out is None else out + piece
    return out


def eight_rows(x):
    missing = 8 - x.shape[0]
    if not missing:
        return x
    return jnp.concatenate([x, jnp.zeros((missing, x.shape[1]), x.dtype)], axis=0)


def bias_line(err, err_at, rows):
    e = err[pl.ds(err_at * 32, rows * 32), :].reshape(rows, 32, -1)
    column = jnp.sum(fold_lanes(jnp.sum(e, axis=0)), axis=1, keepdims=True)
    line = lax.broadcasted_iota(jnp.int32, (32, 128), 0)
    lane = lax.broadcasted_iota(jnp.int32, (32, 128), 1)
    return eight_rows(jnp.sum(jnp.where(lane == line + 96, column, 0.0), axis=0, keepdims=True))


def backward_kernel(
    factor,
    pressure,
    cprev,
    cown,
    clater,
    vprev,
    vown,
    vlater,
    a0h,
    a0l,
    a1h,
    a1l,
    a2h,
    a2l,
    narrow,
    wide,
    out_taps,
    grad_velocity,
    terms,
    e2,
    e1,
    e0,
    eh,
    el,
    weights,
    weights_narrow,
):
    rows, width = vown.shape[1], vown.shape[2]
    a0, a1, a2, split = (a0h, a0l), (a1h, a1l), (a2h, a2l), (eh, el)

    def extended(prev, own, later, c):
        return jnp.concatenate([prev[c, rows - 8 :], own[c], later[c, :8]], axis=0)

    lam = pressure[...]
    adjoint = [
        extended(cprev, cown, clater, 0) - (lam - turn(lam, 1, 0)),
        extended(cprev, cown, clater, 1) - (lam - turn(lam, 1, 1)),
    ]
    v = [extended(vprev, vown, vlater, c) for c in range(2)]
    e3 = [step_size * item for item in adjoint]

    def slope_of(act, at):
        high, low = take(act, at, BLOCK)
        a = high.astype(F32) + low.astype(F32)
        return (1.0 - a * a).reshape(BLOCK, 32, width)

    def keep(ref, at, value):
        put(split, at, value)
        ref[pl.ds(at * 32, BLOCK * 32), :] = value.reshape(BLOCK * 32, width)

    weights_narrow[...] = banded_narrow(narrow[...])
    for s in starts(-3, rows + 6):
        pair = [e3[c][s + 7 : s + 7 + SPAN] for c in range(2)]
        keep(e2, s + 3, narrow_conv(weights_narrow[...], pair) * slope_of(a2, s + 3))
    weights[...] = banded(wide[1])
    for s in starts(-2, rows + 4):
        x = take(split, s + 2, SPAN)
        e1[pl.ds((s + 2) * 32, BLOCK * 32), :] = (
            wide_conv(weights[...], *x) * slope_of(a1, s + 4)
        ).reshape(BLOCK * 32, width)
    split_rows = (rows + 4) * 32
    high, low = halves(e1[...])
    eh[0:split_rows, :] = high
    el[0:split_rows, :] = low
    weights[...] = banded(wide[0])
    for s in starts(-1, rows + 2):
        x = take(split, s + 1, SPAN)
        e0[pl.ds((s + 1) * 32, BLOCK * 32), :] = (
            wide_conv(weights[...], *x) * slope_of(a0, s + 5)
        ).reshape(BLOCK * 32, width)

    own = slice(8, 8 + rows)
    wh, wl = banded_out(out_taps, rows)
    high, low = halves(e0[...])
    cells = (rows + 2) * 32
    wh, wl = wh[:, :cells], wl[:, :cells]
    y = (
        jnp.dot(wh, high, preferred_element_type=F32)
        + jnp.dot(wh, low, preferred_element_type=F32)
        + jnp.dot(wl, high, preferred_element_type=F32)
    )
    through = []
    for c in range(2):
        parts = [y[(2 * q + c) * rows : (2 * q + c + 1) * rows] for q in range(3)]
        through.append(turn(parts[0], 1, 1) + parts[1] + turn(parts[2], -1, 1))

    cross = []
    for k in range(2):
        flux = v[0] * adjoint[k]
        side = v[1][own] * adjoint[k][own]
        cross.append(
            ((turn(flux, -1, 0) - turn(flux, 1, 0)) * 0.5)[own]
            + (turn(side, -1, 1) - turn(side, 1, 1)) * 0.5
        )
    along_x = [((turn(f, -1, 0) - turn(f, 1, 0)) * 0.5)[own] for f in v]
    along_y = [(turn(f[own], -1, 1) - turn(f[own], 1, 1)) * 0.5 for f in v]
    direct = [
        adjoint[0][own] * along_x[0] + adjoint[1][own] * along_x[1],
        adjoint[0][own] * along_y[0] + adjoint[1][own] * along_y[1],
    ]
    for k in range(2):
        grad_velocity[k] = adjoint[k][own] - step_size * (direct[k] - cross[k]) + through[k]

    scale = factor[0, 0]
    middle1 = wide_terms(e2, 3, a1, 4, rows)
    middle0 = wide_terms(e1, 2, a0, 5, rows)

    outer = jnp.concatenate([sided(e3[c][own], 0) for c in range(2)], axis=0)
    lh, ll = halves(outer)
    ah, al = take(a2, 2, rows + 4)
    last = dot_nt(lh, ah) + dot_nt(lh, al) + dot_nt(ll, ah)
    last = last.reshape(6, rows, (rows + 4) * 32)
    group = lax.broadcasted_iota(jnp.int32, (rows, (rows + 4) * 32), 1) // 32
    line = lax.broadcasted_iota(jnp.int32, (rows, (rows + 4) * 32), 0)
    spare = []
    for p in range(3):
        picked = jnp.sum(jnp.where((group == line + p)[None], last, 0.0), axis=1)
        spare.append(eight_rows(lane_groups_summed(picked)))

    inner = jnp.concatenate(
        [jnp.concatenate([turn(f, 1, 1), f, turn(f, -1, 1)], axis=0) for f in v], axis=0
    )
    lh, ll = halves(inner)
    eh0, el0 = high[32 : 32 + rows * 32], low[32 : 32 + rows * 32]
    begin = dot_nt(lh, eh0) + dot_nt(lh, el0) + dot_nt(ll, eh0)
    tall = rows + 16
    begin = begin.reshape(6, tall, rows * 32)
    group = lax.broadcasted_iota(jnp.int32, (tall, rows * 32), 1) // 32
    line = lax.broadcasted_iota(jnp.int32, (tall, rows * 32), 0)
    for p in range(3):
        picked = jnp.sum(jnp.where((line == group + p + 7)[None], begin, 0.0), axis=1)
        spare.append(eight_rows(lane_groups_summed(picked)))

    spare.append(bias_line(e2, 3, rows))
    spare.append(bias_line(e1, 2, rows))
    spare.append(bias_line(e0, 1, rows))
    lane = lax.broadcasted_iota(jnp.int32, (1, 128), 1)
    ends = jnp.zeros((1, 128), F32)
    for c in range(2):
        end = jnp.sum(jnp.sum(e3[c][own], axis=0, keepdims=True), axis=1, keepdims=True)
        ends = ends + jnp.where(lane == 96 + c, end, 0.0)
    spare.append(eight_rows(ends))
    spare.append(jnp.zeros((96 - 8 * len(spare), 128), F32))
    spare = jnp.concatenate(spare, axis=0)
    kept = lax.broadcasted_iota(jnp.int32, (96, 128), 1) < 96
    terms[0:96, :] = jnp.where(kept, middle1, spare) * scale
    terms[96:192, :] = jnp.where(kept, middle0, 0.0) * scale


def unpack_kernel(total, first, bias0, hidden, biases, last, ends):
    for p in range(3):
        for at, begin in enumerate((96, 0)):
            block = total[begin : begin + 96, 32 * p : 32 * p + 32]
            hidden[at, p] = block.reshape(3, 32, 32)
    spare = turn(total[0:96, :], 32, 1)[:, :32]
    for p in range(3):
        for q in range(3):
            for c in range(2):
                at = 8 * p + 3 * c + q
                last[p, q, c : c + 1] = spare[at : at + 1]
                first[p, q, c : c + 1] = spare[24 + at : 25 + at]
    biases[...] = jnp.concatenate([spare[56:57], spare[48:49]], axis=0)
    bias0[...] = spare[64:65]
    ends[...] = spare[72:73, :2]


def total_of(packed):
    lines, lanes = packed.shape
    local = (NEAR, CORE)
    part = packed.reshape(lax.axis_size(local), -1, lanes)
    part = lax.all_to_all(part, local, 0, 0, tiled=True).sum(axis=0)
    part = from_everyone(part, FAR).sum(axis=0)
    return from_everyone(part, local).reshape(lines, lanes)


def forward_taps(w):
    out, into = w.shape[2], w.shape[3]
    return jnp.transpose(w, (1, 2, 0, 3)).reshape(3 * out, 3 * into)


def backward_taps(w):
    out, into = w.shape[2], w.shape[3]
    return jnp.transpose(w[::-1, ::-1], (1, 3, 0, 2)).reshape(3 * into, 3 * out)


def narrow_taps(w):
    t = jnp.transpose(w, (1, 2, 3, 0)).reshape(3 * w.shape[2], 2, 3)
    t = jnp.pad(t, ((0, 0), (0, 0), (0, 5))).reshape(-1, 16)
    return jnp.pad(t, ((0, 0), (0, 112)))


def out_taps_of(w):
    t = jnp.pad(w.reshape(3, 6, w.shape[3]), ((0, 0), (0, 2), (0, 0)))
    return jnp.concatenate([t] * 4, axis=2)


def flipped(w):
    return jnp.swapaxes(w[::-1, ::-1], 2, 3)


def shape_of(*dims, dtype=F32):
    return jax.ShapeDtypeStruct(dims, dtype)


def call(kernel, out_shape, scratch=(), room=63, **extra):
    return pl.pallas_call(
        kernel,
        out_shape=out_shape,
        scratch_shapes=list(scratch),
        compiler_params=pltpu.CompilerParams(vmem_limit_bytes=room * 1024 * 1024),
        **extra,
    )


def body(velocity, cotangent, w_first, b_first, w_hidden, b_hidden, w_last):
    rows, width = velocity.shape[1], velocity.shape[2]
    members = lax.axis_size(GX)
    cprev, clater = shifted(cotangent, GX, 1), shifted(cotangent, GX, -1)
    vprev, vlater = shifted(velocity, GX, 1), shifted(velocity, GX, -1)

    basis, sums = call(
        basis_kernel, (shape_of(ITERS, rows + 16, width), shape_of(members, 128))
    )(cprev, cotangent, clater)
    gathered = lax.all_to_all(sums.reshape(members, 1, 128), GX, 0, 0, tiled=True)

    sums, w_first, b_first, w_hidden, b_hidden, w_last = lax.optimization_barrier(
        (sums, w_first, b_first, w_hidden, b_hidden, w_last)
    )
    wide_pad = ((0, 0), (0, 256 - 96))
    wide = jnp.stack([jnp.pad(forward_taps(w_hidden[m]), wide_pad) for m in range(2)])
    wide_back = jnp.stack([jnp.pad(backward_taps(w_hidden[m]), wide_pad) for m in range(2)])
    narrow = narrow_taps(w_first)
    narrow_back = narrow_taps(flipped(w_last))
    out_taps = out_taps_of(flipped(w_first))
    biases = jnp.stack([b_first, b_hidden[0], b_hidden[1]])
    biases = jnp.broadcast_to(biases[:, :, None], (3, biases.shape[1], 128))

    heights = (rows + 10, rows + 8, rows + 6)
    held = [shape_of(h * 32, width, dtype=BF16) for h in heights for _ in range(2)]
    actives = call(
        forward_kernel,
        tuple(held),
        [
            pltpu.VMEM((96 * BLOCK, 48), BF16),
            pltpu.VMEM((96 * BLOCK, 3 * SPAN * 32), BF16),
            pltpu.VMEM((96 * BLOCK, 3 * SPAN * 32), BF16),
        ],
    )(vprev, velocity, vlater, narrow, wide, biases)

    quick, unsafe = call(
        pressure_kernel, (shape_of(rows + 16, width), shape_of(1, 128, dtype=jnp.int32))
    )(gathered.reshape(members, 128), basis)
    pressure = lax.cond(
        unsafe[0, 0] != 0,
        lambda c, l, _: stepwise_pressure(c, l),
        lambda c, l, q: q,
        cotangent,
        clater,
        quick,
    )

    factor = 1.0 / jnp.sqrt(jnp.float32(members * rows * width))
    whole = pl.BlockSpec(memory_space=pltpu.VMEM)
    grad_velocity, terms = call(
        backward_kernel,
        (shape_of(2, rows, width), shape_of(192, 128)),
        [
            pltpu.VMEM(((rows + 6) * 32, width), F32),
            pltpu.VMEM(((rows + 4) * 32, width), F32),
            pltpu.VMEM(((rows + 2) * 32, width), F32),
            pltpu.VMEM(((rows + 6) * 32, width), BF16),
            pltpu.VMEM(((rows + 6) * 32, width), BF16),
            pltpu.VMEM((96 * BLOCK, 3 * SPAN * 32), BF16),
            pltpu.VMEM((96 * BLOCK, 48), BF16),
        ],
        room=63,
        in_specs=[pl.BlockSpec(memory_space=pltpu.SMEM)] + [whole] * 16,
    )(
        factor.reshape(1, 1),
        pressure,
        cprev,
        cotangent,
        clater,
        vprev,
        velocity,
        vlater,
        *actives,
        narrow_back,
        wide_back,
        out_taps,
    )
    total = total_of(terms)
    taps = w_first.shape[0]
    first, bias0, hidden, biases, last, ends = call(
        unpack_kernel,
        (
            shape_of(taps, taps, 2, 32),
            shape_of(1, 32),
            shape_of(2, taps, taps, 32, 32),
            shape_of(2, 32),
            shape_of(taps, taps, 2, 32),
            shape_of(1, 2),
        ),
    )(total)
    return (
        grad_velocity,
        jnp.swapaxes(first, 2, 3),
        bias0.reshape(-1),
        hidden,
        biases,
        last,
        ends.reshape(-1),
    )


def solution(mesh):
    cores, near = 2, 4
    far = mesh.shape["gx"] // (cores * near)
    finer = Mesh(mesh.devices.reshape(mesh.shape["groups"], far, near, cores), GROUPS_GX)
    placed = (P(None, GROUPS_GX, None), P(None, GROUPS_GX, None), P(), P(), P(), P(), P())
    return jax.shard_map(
        body,
        mesh=finer,
        in_specs=placed,
        out_specs=(
            P(None, GROUPS_GX, None),
            P("groups", None, None, None),
            P("groups"),
            P("groups", None, None, None, None),
            P("groups", None),
            P("groups", None, None, None),
            P("groups"),
        ),
        check_vma=False,
    )
```

```python
import jax
import jax.numpy as jnp
from jax import lax
from jax.experimental import pallas as pl
from jax.experimental.pallas import tpu as pltpu
from jax.sharding import Mesh
from jax.sharding import PartitionSpec as P


ITERS = 8
FAR, NEAR, CORE = "gx_far", "gx_near", "gx_core"
GX = (FAR, NEAR, CORE)
GROUPS_GX = ("groups", FAR, NEAR, CORE)
SPREAD_LIMIT = 3000.0
BLOCK = 6
SPAN = BLOCK + 2
F32 = jnp.float32
BF16 = jnp.bfloat16

step_size = 0.25


def from_everyone(x, axis):
    length = lax.axis_size(axis)
    return lax.all_to_all(jnp.broadcast_to(x[None], (length, *x.shape)), axis, 0, 0, tiled=True)


def shifted(value, axis, steps):
    count = lax.axis_size(axis)
    pairs = [(source, (source + steps) % count) for source in range(count)]
    return lax.ppermute(value, axis, pairs)


def turn(x, steps, axis):
    return pltpu.roll(x, steps % x.shape[axis], axis)


def halves(x):
    high = x.astype(BF16)
    return high, (x - high.astype(F32)).astype(BF16)


def starts(first, count):
    return [min(first + BLOCK * i, first + count - BLOCK) for i in range(-(-count // BLOCK))]


def fold_lanes(x):
    total = x[:, :128]
    for at in range(128, x.shape[1], 128):
        total = total + x[:, at : at + 128]
    return total


def lane_groups_summed(x):
    x = fold_lanes(x)
    x = x + turn(x, 64, 1)
    return x + turn(x, 32, 1)


def neighbours(t):
    return turn(t, 1, 0) + turn(t, -1, 0) + turn(t, 1, 1) + turn(t, -1, 1)


def basis_kernel(prev, own, later, basis, sums, around):
    rows = own.shape[1]
    first = jnp.concatenate([prev[0], own[0], later[0]], axis=0)
    second = jnp.concatenate([prev[1], own[1], later[1]], axis=0)
    source = -(turn(first, -1, 0) - first + (turn(second, -1, 1) - second))
    around[0] = first[rows - 8 : 2 * rows + 8]
    around[1] = second[rows - 8 : 2 * rows + 8]
    line = lax.broadcasted_iota(jnp.int32, (2 * ITERS, 128), 0)
    lane = lax.broadcasted_iota(jnp.int32, (2 * ITERS, 128), 1)
    squares, crosses = [], []

    def product(a, b):
        return fold_lanes(jnp.sum(a[rows : 2 * rows] * b[rows : 2 * rows], axis=0, keepdims=True))

    before, now = None, source
    for k in range(ITERS):
        basis[k] = now[rows - 8 : 2 * rows + 8]
        if k == 0:
            after = -0.25 * neighbours(now)
        else:
            after = -0.5 * neighbours(now) - before
        squares.append(product(now, now))
        crosses.append(product(now, after))
        before, now = now, after
    stacked = jnp.concatenate(squares + crosses, axis=0)
    column = jnp.sum(stacked, axis=1, keepdims=True)
    row = jnp.sum(jnp.where(line == lane, column, 0.0), axis=0, keepdims=True)
    sums[...] = jnp.broadcast_to(row, sums.shape)


def quadratic(a, b, mu):
    total = None
    for i, left in enumerate(a):
        inner = None
        for j, right in enumerate(b):
            term = right * mu[i][j]
            inner = term if inner is None else inner + term
        total = left * inner if total is None else total + left * inner
    return total


def spread(a):
    total = jnp.abs(a[0])
    for item in a[1:]:
        total = total + jnp.abs(item)
    return total


def image_of(c):
    out = [4.0 * item for item in c] + [jnp.zeros_like(c[0])]
    out[1] = out[1] + 4.0 * c[0]
    for k in range(1, len(c)):
        out[k + 1] = out[k + 1] + 2.0 * c[k]
        out[k - 1] = out[k - 1] + 2.0 * c[k]
    return out


def combined(factor, a, b):
    out = []
    for k in range(max(len(a), len(b))):
        if k >= len(a):
            out.append(b[k])
        elif k >= len(b):
            out.append(factor * a[k])
        else:
            out.append(b[k] + factor * a[k])
    return out


def pressure_kernel(gathered, basis, pressure, unsafe):
    total = jnp.sum(gathered[...], axis=0, keepdims=True)
    lane = lax.broadcasted_iota(jnp.int32, (1, 128), 1)
    items = [
        jnp.broadcast_to(jnp.sum(jnp.where(lane == k, total, 0.0), axis=1, keepdims=True), (1, 128))
        for k in range(2 * ITERS)
    ]
    moments = [items[0], items[ITERS]]
    for k in range(1, ITERS):
        moments.append(2.0 * items[k] - items[0])
        moments.append(2.0 * items[ITERS + k] - items[ITERS])
    mu = [
        [0.5 * (moments[i + j] + moments[abs(i - j)]) for j in range(min(ITERS + 1, 2 * ITERS - i))]
        for i in range(ITERS)
    ]
    one = jnp.ones((1, 128), F32)
    residual, direction, answer = [one], [one], [jnp.zeros((1, 128), F32)]
    norm_now = items[0]
    safe = norm_now > 0.0
    for step in range(ITERS):
        image = image_of(direction)
        product = quadratic(direction, image, mu)
        bound = spread(direction) * spread(image) * items[0]
        safe = safe & (product > 0.0) & (bound < SPREAD_LIMIT * product)
        alpha = norm_now / product
        answer = combined(alpha, direction, answer)
        if step + 1 < ITERS:
            residual = combined(-alpha, image, residual)
            norm_next = quadratic(residual, residual, mu)
            size = spread(residual)
            safe = safe & (norm_next > 0.0) & (size * size * items[0] < SPREAD_LIMIT * norm_next)
            direction = combined(norm_next / norm_now, direction, residual)
            norm_now = norm_next
    wide = basis.shape[2] // 128
    lam = None
    for k in range(ITERS):
        term = jnp.concatenate([answer[k]] * wide, axis=1) * basis[k]
        lam = term if lam is None else lam + term
    pressure[...] = lam
    unsafe[0, 0] = jnp.max(jnp.where(safe, 0.0, 1.0)).astype(jnp.int32)


def laplace(field):
    above = shifted(field[-1:], GX, 1)
    below = shifted(field[:1], GX, -1)
    up = jnp.concatenate([above, field[:-1]], axis=0)
    down = jnp.concatenate([field[1:], below], axis=0)
    return 4.0 * field - up - down - jnp.roll(field, 1, 1) - jnp.roll(field, -1, 1)


def sum_of(a, b):
    local = jnp.broadcast_to(jnp.sum(a * b), (1, 128))
    return jnp.sum(from_everyone(local, GX)[:, 0, 0])


def stepwise_pressure(around):
    first, second = around[0, 8:-8], around[1, 8:-8]
    below = around[0, 9:-7]
    source = -(below - first + (jnp.roll(second, -1, 1) - second))

    def iterate(_, carry):
        pressure, residual, direction, norm_now = carry
        image = laplace(direction)
        alpha = norm_now / sum_of(direction, image)
        pressure = pressure + alpha * direction
        residual = residual - alpha * image
        norm_next = sum_of(residual, residual)
        direction = residual + norm_next / norm_now * direction
        return pressure, residual, direction, norm_next

    start = (jnp.zeros_like(source), source, source, sum_of(source, source))
    pressure = lax.fori_loop(0, ITERS, iterate, start)[0]
    above = shifted(pressure[-8:], GX, 1)
    under = shifted(pressure[:8], GX, -1)
    return jnp.concatenate([above, pressure, under], axis=0)


def banded(taps):
    rows = jnp.concatenate([taps] + [turn(taps, 32 * r, 1) for r in range(1, BLOCK)], axis=0)
    high, low = halves(rows)
    return jnp.concatenate([high, high, low], axis=1)


def banded_narrow(taps):
    rows = jnp.concatenate([taps] + [turn(taps, r, 1) for r in range(1, BLOCK)], axis=0)
    high = rows.astype(BF16).astype(F32)
    low = rows - high
    return (high + turn(high, 16, 1) + turn(low, 32, 1)).astype(BF16)[:, :48]


def banded_out(taps, rows):
    width = (rows + 2) * 32
    padded = -(-width // 128)
    lane = lax.broadcasted_iota(jnp.int32, (rows, padded * 128), 1) // 32
    row = lax.broadcasted_iota(jnp.int32, (rows, padded * 128), 0)
    pieces = []
    for j in range(6):
        piece = jnp.zeros((rows, padded * 128), F32)
        for p in range(3):
            line = jnp.concatenate([taps[p][j : j + 1]] * padded, axis=1)
            piece = piece + jnp.where(lane == row + p, line, 0.0)
        pieces.append(piece)
    return halves(jnp.concatenate(pieces, axis=0))


def side_sum(y):
    n = y.shape[1] // 3
    return turn(y[:, :n], 1, 2) + y[:, n : 2 * n] + turn(y[:, 2 * n :], -1, 2)


def wide_conv(weights, high, low):
    x = jnp.concatenate([high, low, high], axis=0)
    y = jnp.dot(weights, x, preferred_element_type=F32)
    return side_sum(y.reshape(BLOCK, 96, y.shape[1]))


def narrow_conv(weights, pair):
    high, low = halves(jnp.concatenate(pair, axis=0))
    x = jnp.concatenate([high, low, high], axis=0)
    y = jnp.dot(weights, x, preferred_element_type=F32)
    return side_sum(y.reshape(BLOCK, 96, y.shape[1]))


def put(refs, at, value):
    high, low = halves(value.reshape(value.shape[0] * 32, value.shape[2]))
    span = pl.ds(at * 32, value.shape[0] * 32)
    refs[0][span, :] = high
    refs[1][span, :] = low


def take(refs, at, rows):
    span = pl.ds(at * 32, rows * 32)
    return refs[0][span, :], refs[1][span, :]


def forward_kernel(
    prev,
    own,
    later,
    narrow,
    wide,
    bias,
    narrow_back,
    wide_back,
    out_taps,
    a0h,
    a0l,
    a1h,
    a1l,
    a2h,
    a2l,
    band2,
    band1,
    band0,
    band_out,
    weights0,
    weights1,
    weights2,
):
    rows, width = own.shape[1], own.shape[2]
    v = [jnp.concatenate([prev[c, rows - 8 :], own[c], later[c, :8]], axis=0) for c in range(2)]
    weights0[...] = banded_narrow(narrow[...])
    weights1[...] = banded(wide[0])
    weights2[...] = banded(wide[1])
    shift = [jnp.concatenate([bias[m]] * (width // 128), axis=1) for m in range(3)]
    for s in starts(-5, rows + 10):
        pair = [v[c][s + 7 : s + 7 + SPAN] for c in range(2)]
        put((a0h, a0l), s + 5, jnp.tanh(narrow_conv(weights0[...], pair) + shift[0]))
    for s in starts(-4, rows + 8):
        x = take((a0h, a0l), s + 4, SPAN)
        put((a1h, a1l), s + 4, jnp.tanh(wide_conv(weights1[...], *x) + shift[1]))
    for s in starts(-3, rows + 6):
        x = take((a1h, a1l), s + 3, SPAN)
        put((a2h, a2l), s + 3, jnp.tanh(wide_conv(weights2[...], *x) + shift[2]))
    band2[...] = banded_narrow(narrow_back[...])
    band1[...] = banded(wide_back[1])
    band0[...] = banded(wide_back[0])
    high, low = banded_out(out_taps[...], rows)
    band_out[0] = high
    band_out[1] = low


def dot_nt(a, b):
    return lax.dot_general(a, b, (((1,), (1,)), ((), ())), preferred_element_type=F32)


def sided(e, axis):
    return jnp.concatenate([turn(e, -1, e.ndim - 1), e, turn(e, 1, e.ndim - 1)], axis=axis)


def wide_terms(err, err_at, act, act_at, rows):
    total = None
    lines = -(-rows // BLOCK)
    for i in range(lines):
        s = min(BLOCK * i, rows - BLOCK)
        e = err[pl.ds((err_at + s) * 32, BLOCK * 32), :].reshape(BLOCK, 32, -1)
        spent = BLOCK * i - s
        if spent:
            e = jnp.concatenate([jnp.zeros_like(e[:spent]), e[spent:]], axis=0)
        high, low = halves(sided(e, 1).reshape(BLOCK * 96, -1))
        ah, al = take(act, act_at + s - 1, SPAN)
        term = dot_nt(
            jnp.concatenate([high, high, low], axis=1), jnp.concatenate([ah, al, ah], axis=1)
        )
        total = term if total is None else total + term
    total = total.reshape(BLOCK, 96, SPAN * 32)
    out = None
    for r in range(BLOCK):
        piece = turn(total[r], -32 * r, 1)[:, :128]
        out = piece if out is None else out + piece
    return out


def eight_rows(x):
    missing = 8 - x.shape[0]
    if not missing:
        return x
    return jnp.concatenate([x, jnp.zeros((missing, x.shape[1]), x.dtype)], axis=0)


def bias_line(err, err_at, rows):
    e = err[pl.ds(err_at * 32, rows * 32), :].reshape(rows, 32, -1)
    column = jnp.sum(fold_lanes(jnp.sum(e, axis=0)), axis=1, keepdims=True)
    line = lax.broadcasted_iota(jnp.int32, (32, 128), 0)
    lane = lax.broadcasted_iota(jnp.int32, (32, 128), 1)
    return jnp.sum(jnp.where(lane == line + 96, column, 0.0), axis=0, keepdims=True)


def backward_kernel(
    factor,
    pressure,
    around,
    vprev,
    vown,
    vlater,
    far2,
    far2h,
    far2l,
    far1,
    far1h,
    far1l,
    far0,
    far0h,
    far0l,
    far_out,
    grad_velocity,
    terms,
    e2,
    e1,
    e0,
    eh,
    el,
    band2,
    a2h,
    a2l,
    band1,
    a1h,
    a1l,
    band0,
    a0h,
    a0l,
    band_out,
    arrived,
):
    rows, width = vown.shape[1], vown.shape[2]
    a0, a1, a2, split = (a0h, a0l), (a1h, a1l), (a2h, a2l), (eh, el)
    sources = (far2, far2h, far2l, far1, far1h, far1l, far0, far0h, far0l, far_out)
    targets = (band2, a2h, a2l, band1, a1h, a1l, band0, a0h, a0l, band_out)
    copies = [
        pltpu.make_async_copy(source, target, arrived.at[i])
        for i, (source, target) in enumerate(zip(sources, targets))
    ]
    for copy in copies:
        copy.start()

    lam = pressure[...]
    adjoint = [around[0] - (lam - turn(lam, 1, 0)), around[1] - (lam - turn(lam, 1, 1))]
    v = [jnp.concatenate([vprev[c, rows - 8 :], vown[c], vlater[c, :8]], axis=0) for c in range(2)]
    e3 = [step_size * item for item in adjoint]

    def slope_of(act, at):
        high, low = take(act, at, BLOCK)
        a = high.astype(F32) + low.astype(F32)
        return (1.0 - a * a).reshape(BLOCK, 32, width)

    def keep(ref, at, value):
        put(split, at, value)
        ref[pl.ds(at * 32, BLOCK * 32), :] = value.reshape(BLOCK * 32, width)

    for copy in copies[:3]:
        copy.wait()
    for s in starts(-3, rows + 6):
        pair = [e3[c][s + 7 : s + 7 + SPAN] for c in range(2)]
        keep(e2, s + 3, narrow_conv(band2[...], pair) * slope_of(a2, s + 3))
    for copy in copies[3:6]:
        copy.wait()
    for s in starts(-2, rows + 4):
        x = take(split, s + 2, SPAN)
        e1[pl.ds((s + 2) * 32, BLOCK * 32), :] = (
            wide_conv(band1[...], *x) * slope_of(a1, s + 4)
        ).reshape(BLOCK * 32, width)
    split_rows = (rows + 4) * 32
    high, low = halves(e1[...])
    eh[0:split_rows, :] = high
    el[0:split_rows, :] = low
    for copy in copies[6:]:
        copy.wait()
    for s in starts(-1, rows + 2):
        x = take(split, s + 1, SPAN)
        e0[pl.ds((s + 1) * 32, BLOCK * 32), :] = (
            wide_conv(band0[...], *x) * slope_of(a0, s + 5)
        ).reshape(BLOCK * 32, width)

    own = slice(8, 8 + rows)
    high, low = halves(e0[...])
    cells = (rows + 2) * 32
    wh, wl = band_out[0, :, :cells], band_out[1, :, :cells]
    y = (
        jnp.dot(wh, high, preferred_element_type=F32)
        + jnp.dot(wh, low, preferred_element_type=F32)
        + jnp.dot(wl, high, preferred_element_type=F32)
    )
    through = []
    for c in range(2):
        parts = [y[(2 * q + c) * rows : (2 * q + c + 1) * rows] for q in range(3)]
        through.append(turn(parts[0], 1, 1) + parts[1] + turn(parts[2], -1, 1))

    cross = []
    for k in range(2):
        flux = v[0] * adjoint[k]
        side = v[1][own] * adjoint[k][own]
        cross.append(
            ((turn(flux, -1, 0) - turn(flux, 1, 0)) * 0.5)[own]
            + (turn(side, -1, 1) - turn(side, 1, 1)) * 0.5
        )
    along_x = [((turn(f, -1, 0) - turn(f, 1, 0)) * 0.5)[own] for f in v]
    along_y = [(turn(f[own], -1, 1) - turn(f[own], 1, 1)) * 0.5 for f in v]
    direct = [
        adjoint[0][own] * along_x[0] + adjoint[1][own] * along_x[1],
        adjoint[0][own] * along_y[0] + adjoint[1][own] * along_y[1],
    ]
    for k in range(2):
        grad_velocity[k] = adjoint[k][own] - step_size * (direct[k] - cross[k]) + through[k]

    scale = factor[0, 0]
    middle1 = wide_terms(e2, 3, a1, 4, rows)
    middle0 = wide_terms(e1, 2, a0, 5, rows)

    outer = jnp.concatenate([sided(e3[c][own], 0) for c in range(2)], axis=0)
    lh, ll = halves(outer)
    ah, al = take(a2, 2, rows + 4)
    last = dot_nt(lh, ah) + dot_nt(lh, al) + dot_nt(ll, ah)
    last = last.reshape(6, rows, (rows + 4) * 32)
    group = lax.broadcasted_iota(jnp.int32, (rows, (rows + 4) * 32), 1) // 32
    line = lax.broadcasted_iota(jnp.int32, (rows, (rows + 4) * 32), 0)
    last = [
        eight_rows(
            lane_groups_summed(
                jnp.sum(jnp.where((group == line + p)[None], last, 0.0), axis=1)
            )
        )
        for p in range(3)
    ]

    inner = jnp.concatenate(
        [jnp.concatenate([turn(f, 1, 1), f, turn(f, -1, 1)], axis=0) for f in v], axis=0
    )
    lh, ll = halves(inner)
    eh0, el0 = high[32 : 32 + rows * 32], low[32 : 32 + rows * 32]
    begin = dot_nt(lh, eh0) + dot_nt(lh, el0) + dot_nt(ll, eh0)
    tall = rows + 16
    begin = begin.reshape(6, tall, rows * 32)
    group = lax.broadcasted_iota(jnp.int32, (tall, rows * 32), 1) // 32
    line = lax.broadcasted_iota(jnp.int32, (tall, rows * 32), 0)
    begin = [
        eight_rows(
            lane_groups_summed(
                jnp.sum(jnp.where((line == group + p + 7)[None], begin, 0.0), axis=1)
            )
        )
        for p in range(3)
    ]

    lane = lax.broadcasted_iota(jnp.int32, (1, 128), 1)
    ends = jnp.zeros((1, 128), F32)
    for c in range(2):
        end = jnp.sum(jnp.sum(e3[c][own], axis=0, keepdims=True), axis=1, keepdims=True)
        ends = ends + jnp.where(lane == 96 + c, end, 0.0)
    sums = [bias_line(e2, 3, rows), bias_line(e1, 2, rows), bias_line(e0, 1, rows), ends]
    sums = eight_rows(jnp.concatenate(sums, axis=0))
    place = lax.broadcasted_iota(jnp.int32, (8, 128), 1) // 32

    def merged(parts, rest):
        for p, part in enumerate(parts):
            rest = jnp.where(place == p, part, rest)
        return rest

    terms[0:72, :] = dense(middle1) * scale
    terms[72:144, :] = dense(middle0) * scale
    terms[144:152, :] = merged(last, sums) * scale
    terms[152:160, :] = merged(begin, jnp.zeros_like(sums)) * scale


def dense(x):
    flat = jnp.concatenate([x[:, 32 * p : 32 * p + 32] for p in range(3)], axis=0)
    return jnp.concatenate([flat[72 * g : 72 * g + 72] for g in range(4)], axis=1)


def sparse(x):
    flat = jnp.concatenate([x[:, 32 * g : 32 * g + 32] for g in range(4)], axis=0)
    return [flat[96 * p : 96 * p + 96] for p in range(3)]


def unpack_kernel(total, first, bias0, hidden, biases, last, ends):
    for at, begin in enumerate((72, 0)):
        for p, block in enumerate(sparse(total[begin : begin + 72, :])):
            hidden[at, p] = block.reshape(3, 32, 32)
    for p in range(3):
        for ref, begin in ((last, 144), (first, 152)):
            part = total[begin : begin + 8, 32 * p : 32 * p + 32]
            for q in range(3):
                ref[p, q] = jnp.concatenate([part[q : q + 1], part[3 + q : 4 + q]], axis=0)
    sums = total[144:152, 96:128]
    biases[...] = jnp.concatenate([sums[1:2], sums[0:1]], axis=0)
    bias0[...] = sums[2:3]
    ends[...] = sums[3:4, :2]


def total_of(packed):
    lines, lanes = packed.shape
    local = (NEAR, CORE)
    part = packed.reshape(lax.axis_size(local), -1, lanes)
    part = lax.all_to_all(part, local, 0, 0, tiled=True).sum(axis=0)
    part = from_everyone(part, FAR).sum(axis=0)
    return from_everyone(part, local).reshape(lines, lanes)


def forward_taps(w):
    out, into = w.shape[2], w.shape[3]
    return jnp.transpose(w, (1, 2, 0, 3)).reshape(3 * out, 3 * into)


def backward_taps(w):
    out, into = w.shape[2], w.shape[3]
    return jnp.transpose(w[::-1, ::-1], (1, 3, 0, 2)).reshape(3 * into, 3 * out)


def narrow_taps(w):
    t = jnp.transpose(w, (1, 2, 3, 0)).reshape(3 * w.shape[2], 2, 3)
    t = jnp.pad(t, ((0, 0), (0, 0), (0, 5))).reshape(-1, 16)
    return jnp.pad(t, ((0, 0), (0, 112)))


def out_taps_of(w):
    t = jnp.pad(w.reshape(3, 6, w.shape[3]), ((0, 0), (0, 2), (0, 0)))
    return jnp.concatenate([t] * 4, axis=2)


def flipped(w):
    return jnp.swapaxes(w[::-1, ::-1], 2, 3)


def shape_of(*dims, dtype=F32):
    return jax.ShapeDtypeStruct(dims, dtype)


def call(kernel, out_shape, scratch=(), room=63, **extra):
    return pl.pallas_call(
        kernel,
        out_shape=out_shape,
        scratch_shapes=list(scratch),
        compiler_params=pltpu.CompilerParams(vmem_limit_bytes=room * 1024 * 1024),
        **extra,
    )


def body(velocity, cotangent, w_first, b_first, w_hidden, b_hidden, w_last):
    rows, width = velocity.shape[1], velocity.shape[2]
    members = lax.axis_size(GX)
    cprev, clater = shifted(cotangent, GX, 1), shifted(cotangent, GX, -1)
    basis, sums, around = call(
        basis_kernel,
        (
            shape_of(ITERS, rows + 16, width),
            shape_of(members, 128),
            shape_of(2, rows + 16, width),
        ),
        room=16,
    )(cprev, cotangent, clater)
    gathered = lax.all_to_all(sums.reshape(members, 1, 128), GX, 0, 0, tiled=True)

    sums, w_first, b_first, w_hidden, b_hidden, w_last = lax.optimization_barrier(
        (sums, w_first, b_first, w_hidden, b_hidden, w_last)
    )
    sums, velocity = lax.optimization_barrier((sums, velocity))
    vprev, vlater = shifted(velocity, GX, 1), shifted(velocity, GX, -1)
    wide_pad = ((0, 0), (0, 256 - 96))
    wide = jnp.stack([jnp.pad(forward_taps(w_hidden[m]), wide_pad) for m in range(2)])
    wide_back = jnp.stack([jnp.pad(backward_taps(w_hidden[m]), wide_pad) for m in range(2)])
    narrow = narrow_taps(w_first)
    narrow_back = narrow_taps(flipped(w_last))
    out_taps = out_taps_of(flipped(w_first))
    biases = jnp.stack([b_first, b_hidden[0], b_hidden[1]])
    biases = jnp.broadcast_to(biases[:, :, None], (3, biases.shape[1], 128))

    heights = (rows + 10, rows + 8, rows + 6)
    held = [shape_of(h * 32, width, dtype=BF16) for h in heights for _ in range(2)]
    wide_band = shape_of(96 * BLOCK, 3 * SPAN * 32, dtype=BF16)
    narrow_band = shape_of(96 * BLOCK, 48, dtype=BF16)
    edge = -(-(rows + 2) * 32 // 128) * 128
    held += [narrow_band, wide_band, wide_band, shape_of(2, 6 * rows, edge, dtype=BF16)]
    a0h, a0l, a1h, a1l, a2h, a2l, band2, band1, band0, band_out = call(
        forward_kernel,
        tuple(held),
        [pltpu.VMEM(item.shape, item.dtype) for item in (narrow_band, wide_band, wide_band)],
    )(vprev, velocity, vlater, narrow, wide, biases, narrow_back, wide_back, out_taps)

    quick, unsafe = call(
        pressure_kernel,
        (shape_of(rows + 16, width), shape_of(1, 1, dtype=jnp.int32)),
        room=12,
        out_specs=(
            pl.BlockSpec(memory_space=pltpu.VMEM),
            pl.BlockSpec(memory_space=pltpu.SMEM),
        ),
    )(gathered.reshape(members, 128), basis)
    pressure = lax.cond(
        unsafe[0, 0] != 0,
        lambda c, _: stepwise_pressure(c),
        lambda c, q: q,
        around,
        quick,
    )

    factor = 1.0 / jnp.sqrt(jnp.float32(members * rows * width))
    whole = pl.BlockSpec(memory_space=pltpu.VMEM)
    outside = pl.BlockSpec(memory_space=pl.ANY)
    fetched = (band2, a2h, a2l, band1, a1h, a1l, band0, a0h, a0l, band_out)
    grad_velocity, terms = call(
        backward_kernel,
        (shape_of(2, rows, width), shape_of(160, 128)),
        [
            pltpu.VMEM(((rows + 6) * 32, width), F32),
            pltpu.VMEM(((rows + 4) * 32, width), F32),
            pltpu.VMEM(((rows + 2) * 32, width), F32),
            pltpu.VMEM(((rows + 6) * 32, width), BF16),
            pltpu.VMEM(((rows + 6) * 32, width), BF16),
        ]
        + [pltpu.VMEM(item.shape, item.dtype) for item in fetched]
        + [pltpu.SemaphoreType.DMA((len(fetched),))],
        in_specs=[pl.BlockSpec(memory_space=pltpu.SMEM)] + [whole] * 5 + [outside] * len(fetched),
    )(factor.reshape(1, 1), pressure, around, vprev, velocity, vlater, *fetched)
    total = total_of(terms)
    taps = w_first.shape[0]
    first, bias0, hidden, biases, last, ends = call(
        unpack_kernel,
        (
            shape_of(taps, taps, 2, 32),
            shape_of(1, 32),
            shape_of(2, taps, taps, 32, 32),
            shape_of(2, 32),
            shape_of(taps, taps, 2, 32),
            shape_of(1, 2),
        ),
    )(total)
    return (
        grad_velocity,
        jnp.swapaxes(first, 2, 3),
        bias0.reshape(-1),
        hidden,
        biases,
        last,
        ends.reshape(-1),
    )


def solution(mesh):
    cores, near = 2, 4
    far = mesh.shape["gx"] // (cores * near)
    finer = Mesh(mesh.devices.reshape(mesh.shape["groups"], far, near, cores), GROUPS_GX)
    placed = (P(None, GROUPS_GX, None), P(None, GROUPS_GX, None), P(), P(), P(), P(), P())
    return jax.shard_map(
        body,
        mesh=finer,
        in_specs=placed,
        out_specs=(
            P(None, GROUPS_GX, None),
            P("groups", None, None, None),
            P("groups"),
            P("groups", None, None, None, None),
            P("groups", None),
            P("groups", None, None, None),
            P("groups"),
        ),
        check_vma=False,
    )
```

```python
import jax
import jax.numpy as jnp
from jax import lax
from jax.experimental import pallas as pl
from jax.experimental.pallas import tpu as pltpu
from jax.sharding import Mesh
from jax.sharding import PartitionSpec as P


ITERS = 8
FAR, NEAR, CORE = "gx_far", "gx_near", "gx_core"
GX = (FAR, NEAR, CORE)
GROUPS_GX = ("groups", FAR, NEAR, CORE)
SPREAD_LIMIT = 3000.0
BLOCK = 6
SPAN = BLOCK + 2
F32 = jnp.float32
BF16 = jnp.bfloat16

step_size = 0.25


def from_everyone(x, axis):
    length = lax.axis_size(axis)
    return lax.all_to_all(jnp.broadcast_to(x[None], (length, *x.shape)), axis, 0, 0, tiled=True)


def shifted(value, axis, steps):
    count = lax.axis_size(axis)
    pairs = [(source, (source + steps) % count) for source in range(count)]
    return lax.ppermute(value, axis, pairs)


def turn(x, steps, axis):
    return pltpu.roll(x, steps % x.shape[axis], axis)


def halves(x):
    high = x.astype(BF16)
    return high, (x - high.astype(F32)).astype(BF16)


def starts(first, count):
    return [min(first + BLOCK * i, first + count - BLOCK) for i in range(-(-count // BLOCK))]


def fold_lanes(x):
    total = x[:, :128]
    for at in range(128, x.shape[1], 128):
        total = total + x[:, at : at + 128]
    return total


def lane_groups_summed(x):
    x = fold_lanes(x)
    x = x + turn(x, 64, 1)
    return x + turn(x, 32, 1)


def neighbours(t):
    return turn(t, 1, 0) + turn(t, -1, 0) + turn(t, 1, 1) + turn(t, -1, 1)


def basis_kernel(prev, own, later, basis, sums, around):
    rows = own.shape[1]
    first = jnp.concatenate([prev[0], own[0], later[0]], axis=0)
    second = jnp.concatenate([prev[1], own[1], later[1]], axis=0)
    source = -(turn(first, -1, 0) - first + (turn(second, -1, 1) - second))
    around[0] = first[rows - 8 : 2 * rows + 8]
    around[1] = second[rows - 8 : 2 * rows + 8]
    line = lax.broadcasted_iota(jnp.int32, (2 * ITERS, 128), 0)
    lane = lax.broadcasted_iota(jnp.int32, (2 * ITERS, 128), 1)
    squares, crosses = [], []

    def product(a, b):
        return fold_lanes(jnp.sum(a[rows : 2 * rows] * b[rows : 2 * rows], axis=0, keepdims=True))

    before, now = None, source
    for k in range(ITERS):
        basis[k] = now[rows - 8 : 2 * rows + 8]
        if k == 0:
            after = -0.25 * neighbours(now)
        else:
            after = -0.5 * neighbours(now) - before
        squares.append(product(now, now))
        crosses.append(product(now, after))
        before, now = now, after
    stacked = jnp.concatenate(squares + crosses, axis=0)
    column = jnp.sum(stacked, axis=1, keepdims=True)
    row = jnp.sum(jnp.where(line == lane, column, 0.0), axis=0, keepdims=True)
    sums[...] = jnp.broadcast_to(row, sums.shape)


def quadratic(a, b, mu):
    total = None
    for i, left in enumerate(a):
        inner = None
        for j, right in enumerate(b):
            term = right * mu[i][j]
            inner = term if inner is None else inner + term
        total = left * inner if total is None else total + left * inner
    return total


def spread(a):
    total = jnp.abs(a[0])
    for item in a[1:]:
        total = total + jnp.abs(item)
    return total


def image_of(c):
    out = [4.0 * item for item in c] + [jnp.zeros_like(c[0])]
    out[1] = out[1] + 4.0 * c[0]
    for k in range(1, len(c)):
        out[k + 1] = out[k + 1] + 2.0 * c[k]
        out[k - 1] = out[k - 1] + 2.0 * c[k]
    return out


def combined(factor, a, b):
    out = []
    for k in range(max(len(a), len(b))):
        if k >= len(a):
            out.append(b[k])
        elif k >= len(b):
            out.append(factor * a[k])
        else:
            out.append(b[k] + factor * a[k])
    return out


def pressure_kernel(gathered, basis, pressure, unsafe):
    total = jnp.sum(gathered[...], axis=0, keepdims=True)
    lane = lax.broadcasted_iota(jnp.int32, (1, 128), 1)
    items = [
        jnp.broadcast_to(jnp.sum(jnp.where(lane == k, total, 0.0), axis=1, keepdims=True), (1, 128))
        for k in range(2 * ITERS)
    ]
    moments = [items[0], items[ITERS]]
    for k in range(1, ITERS):
        moments.append(2.0 * items[k] - items[0])
        moments.append(2.0 * items[ITERS + k] - items[ITERS])
    mu = [
        [0.5 * (moments[i + j] + moments[abs(i - j)]) for j in range(min(ITERS + 1, 2 * ITERS - i))]
        for i in range(ITERS)
    ]
    one = jnp.ones((1, 128), F32)
    residual, direction, answer = [one], [one], [jnp.zeros((1, 128), F32)]
    norm_now = items[0]
    safe = norm_now > 0.0
    for step in range(ITERS):
        image = image_of(direction)
        product = quadratic(direction, image, mu)
        bound = spread(direction) * spread(image) * items[0]
        safe = safe & (product > 0.0) & (bound < SPREAD_LIMIT * product)
        alpha = norm_now / product
        answer = combined(alpha, direction, answer)
        if step + 1 < ITERS:
            residual = combined(-alpha, image, residual)
            norm_next = quadratic(residual, residual, mu)
            size = spread(residual)
            safe = safe & (norm_next > 0.0) & (size * size * items[0] < SPREAD_LIMIT * norm_next)
            direction = combined(norm_next / norm_now, direction, residual)
            norm_now = norm_next
    wide = basis.shape[2] // 128
    lam = None
    for k in range(ITERS):
        term = jnp.concatenate([answer[k]] * wide, axis=1) * basis[k]
        lam = term if lam is None else lam + term
    pressure[...] = lam
    unsafe[0, 0] = jnp.max(jnp.where(safe, 0.0, 1.0)).astype(jnp.int32)


def laplace(field):
    above = shifted(field[-1:], GX, 1)
    below = shifted(field[:1], GX, -1)
    up = jnp.concatenate([above, field[:-1]], axis=0)
    down = jnp.concatenate([field[1:], below], axis=0)
    return 4.0 * field - up - down - jnp.roll(field, 1, 1) - jnp.roll(field, -1, 1)


def sum_of(a, b):
    local = jnp.broadcast_to(jnp.sum(a * b), (1, 128))
    return jnp.sum(from_everyone(local, GX)[:, 0, 0])


def stepwise_pressure(around):
    first, second = around[0, 8:-8], around[1, 8:-8]
    below = around[0, 9:-7]
    source = -(below - first + (jnp.roll(second, -1, 1) - second))

    def iterate(_, carry):
        pressure, residual, direction, norm_now = carry
        image = laplace(direction)
        alpha = norm_now / sum_of(direction, image)
        pressure = pressure + alpha * direction
        residual = residual - alpha * image
        norm_next = sum_of(residual, residual)
        direction = residual + norm_next / norm_now * direction
        return pressure, residual, direction, norm_next

    start = (jnp.zeros_like(source), source, source, sum_of(source, source))
    pressure = lax.fori_loop(0, ITERS, iterate, start)[0]
    above = shifted(pressure[-8:], GX, 1)
    under = shifted(pressure[:8], GX, -1)
    return jnp.concatenate([above, pressure, under], axis=0)


def banded(taps):
    rows = jnp.concatenate([taps] + [turn(taps, 32 * r, 1) for r in range(1, BLOCK)], axis=0)
    high, low = halves(rows)
    return jnp.concatenate([high, high, low], axis=1)


def banded_narrow(taps):
    rows = jnp.concatenate([taps] + [turn(taps, r, 1) for r in range(1, BLOCK)], axis=0)
    high, low = halves(rows)
    return jnp.concatenate([high[:, :48], high[:, :48], low[:, :48]], axis=1)


def banded_out(taps, rows):
    width = (rows + 2) * 32
    padded = -(-width // 128)
    lane = lax.broadcasted_iota(jnp.int32, (rows, padded * 128), 1) // 32
    row = lax.broadcasted_iota(jnp.int32, (rows, padded * 128), 0)
    pieces = []
    for j in range(6):
        piece = jnp.zeros((rows, padded * 128), F32)
        for p in range(3):
            line = jnp.concatenate([taps[p][j : j + 1]] * padded, axis=1)
            piece = piece + jnp.where(lane == row + p, line, 0.0)
        pieces.append(piece)
    return halves(jnp.concatenate(pieces, axis=0))


def side_sum(y):
    n = y.shape[1] // 3
    return turn(y[:, :n], 1, 2) + y[:, n : 2 * n] + turn(y[:, 2 * n :], -1, 2)


def wide_conv(weights, high, low):
    x = jnp.concatenate([high, low, high], axis=0)
    y = jnp.dot(weights, x, preferred_element_type=F32)
    return side_sum(y.reshape(BLOCK, 96, y.shape[1]))


def narrow_conv(weights, pair):
    x = jnp.concatenate(pair, axis=0)
    high, low = halves(jnp.concatenate([turn(x, 1, 1), x, turn(x, -1, 1)], axis=0))
    x = jnp.concatenate([high, low, high], axis=0)
    y = jnp.dot(weights, x, preferred_element_type=F32)
    return y.reshape(BLOCK, 32, y.shape[1])


def put(refs, at, value):
    high, low = halves(value.reshape(value.shape[0] * 32, value.shape[2]))
    span = pl.ds(at * 32, value.shape[0] * 32)
    refs[0][span, :] = high
    refs[1][span, :] = low


def take(refs, at, rows):
    span = pl.ds(at * 32, rows * 32)
    return refs[0][span, :], refs[1][span, :]


def forward_kernel(
    prev,
    own,
    later,
    narrow,
    wide,
    bias,
    narrow_back,
    wide_back,
    out_taps,
    a0h,
    a0l,
    a1h,
    a1l,
    a2h,
    a2l,
    band2,
    band1,
    band0,
    band_out,
    weights0,
    weights1,
    weights2,
):
    rows, width = own.shape[1], own.shape[2]
    v = [jnp.concatenate([prev[c, rows - 8 :], own[c], later[c, :8]], axis=0) for c in range(2)]
    weights0[...] = banded_narrow(narrow[...])
    weights1[...] = banded(wide[0])
    weights2[...] = banded(wide[1])
    shift = [jnp.concatenate([bias[m]] * (width // 128), axis=1) for m in range(3)]
    for s in starts(-5, rows + 10):
        pair = [v[c][s + 7 : s + 7 + SPAN] for c in range(2)]
        put((a0h, a0l), s + 5, jnp.tanh(narrow_conv(weights0[...], pair) + shift[0]))
    for s in starts(-4, rows + 8):
        x = take((a0h, a0l), s + 4, SPAN)
        put((a1h, a1l), s + 4, jnp.tanh(wide_conv(weights1[...], *x) + shift[1]))
    for s in starts(-3, rows + 6):
        x = take((a1h, a1l), s + 3, SPAN)
        put((a2h, a2l), s + 3, jnp.tanh(wide_conv(weights2[...], *x) + shift[2]))
    band2[...] = banded_narrow(narrow_back[...])
    band1[...] = banded(wide_back[1])
    band0[...] = banded(wide_back[0])
    high, low = banded_out(out_taps[...], rows)
    band_out[0] = high
    band_out[1] = low


def dot_nt(a, b):
    return lax.dot_general(a, b, (((1,), (1,)), ((), ())), preferred_element_type=F32)


def sided(e, axis):
    return jnp.concatenate([turn(e, -1, e.ndim - 1), e, turn(e, 1, e.ndim - 1)], axis=axis)


def wide_terms(err, err_at, act, act_at, rows):
    total = None
    lines = -(-rows // BLOCK)
    for i in range(lines):
        s = min(BLOCK * i, rows - BLOCK)
        e = err[pl.ds((err_at + s) * 32, BLOCK * 32), :].reshape(BLOCK, 32, -1)
        spent = BLOCK * i - s
        if spent:
            e = jnp.concatenate([jnp.zeros_like(e[:spent]), e[spent:]], axis=0)
        high, low = halves(sided(e, 1).reshape(BLOCK * 96, -1))
        ah, al = take(act, act_at + s - 1, SPAN)
        term = dot_nt(
            jnp.concatenate([high, high, low], axis=1), jnp.concatenate([ah, al, ah], axis=1)
        )
        total = term if total is None else total + term
    total = total.reshape(BLOCK, 96, SPAN * 32)
    out = None
    for r in range(BLOCK):
        piece = turn(total[r], -32 * r, 1)[:, :128]
        out = piece if out is None else out + piece
    return out


def eight_rows(x):
    missing = 8 - x.shape[0]
    if not missing:
        return x
    return jnp.concatenate([x, jnp.zeros((missing, x.shape[1]), x.dtype)], axis=0)


def bias_line(err, err_at, rows):
    e = err[pl.ds(err_at * 32, rows * 32), :].reshape(rows, 32, -1)
    column = jnp.sum(fold_lanes(jnp.sum(e, axis=0)), axis=1, keepdims=True)
    line = lax.broadcasted_iota(jnp.int32, (32, 128), 0)
    lane = lax.broadcasted_iota(jnp.int32, (32, 128), 1)
    return jnp.sum(jnp.where(lane == line + 96, column, 0.0), axis=0, keepdims=True)


def backward_kernel(
    factor,
    pressure,
    around,
    vprev,
    vown,
    vlater,
    far2,
    far2h,
    far2l,
    far1,
    far1h,
    far1l,
    far0,
    far0h,
    far0l,
    far_out,
    grad_velocity,
    terms,
    e2,
    e1,
    e0,
    eh,
    el,
    fh,
    fl,
    band2,
    a2h,
    a2l,
    band1,
    a1h,
    a1l,
    band0,
    a0h,
    a0l,
    band_out,
    arrived,
):
    rows, width = vown.shape[1], vown.shape[2]
    a0, a1, a2, split = (a0h, a0l), (a1h, a1l), (a2h, a2l), (eh, el)
    other = (fh, fl)
    sources = (far2, far2h, far2l, far1, far1h, far1l, far0, far0h, far0l, far_out)
    targets = (band2, a2h, a2l, band1, a1h, a1l, band0, a0h, a0l, band_out)
    copies = [
        pltpu.make_async_copy(source, target, arrived.at[i])
        for i, (source, target) in enumerate(zip(sources, targets))
    ]
    for copy in copies:
        copy.start()

    lam = pressure[...]
    adjoint = [around[0] - (lam - turn(lam, 1, 0)), around[1] - (lam - turn(lam, 1, 1))]
    v = [jnp.concatenate([vprev[c, rows - 8 :], vown[c], vlater[c, :8]], axis=0) for c in range(2)]
    e3 = [step_size * item for item in adjoint]

    def slope_of(act, at):
        high, low = take(act, at, BLOCK)
        a = high.astype(F32) + low.astype(F32)
        return (1.0 - a * a).reshape(BLOCK, 32, width)

    def keep(ref, parts, at, value):
        put(parts, at, value)
        ref[pl.ds(at * 32, BLOCK * 32), :] = value.reshape(BLOCK * 32, width)

    for copy in copies[:3]:
        copy.wait()
    for s in starts(-3, rows + 6):
        pair = [e3[c][s + 7 : s + 7 + SPAN] for c in range(2)]
        keep(e2, split, s + 3, narrow_conv(band2[...], pair) * slope_of(a2, s + 3))
    for copy in copies[3:6]:
        copy.wait()
    for s in starts(-2, rows + 4):
        x = take(split, s + 2, SPAN)
        keep(e1, other, s + 2, wide_conv(band1[...], *x) * slope_of(a1, s + 4))
    for copy in copies[6:]:
        copy.wait()
    for s in starts(-1, rows + 2):
        x = take(other, s + 1, SPAN)
        keep(e0, split, s + 1, wide_conv(band0[...], *x) * slope_of(a0, s + 5))

    own = slice(8, 8 + rows)
    cells = (rows + 2) * 32
    high, low = eh[0:cells, :], el[0:cells, :]
    wh, wl = band_out[0, :, :cells], band_out[1, :, :cells]
    y = (
        jnp.dot(wh, high, preferred_element_type=F32)
        + jnp.dot(wh, low, preferred_element_type=F32)
        + jnp.dot(wl, high, preferred_element_type=F32)
    )
    through = []
    for c in range(2):
        parts = [y[(2 * q + c) * rows : (2 * q + c + 1) * rows] for q in range(3)]
        through.append(turn(parts[0], 1, 1) + parts[1] + turn(parts[2], -1, 1))

    cross = []
    for k in range(2):
        flux = v[0] * adjoint[k]
        side = v[1][own] * adjoint[k][own]
        cross.append(
            ((turn(flux, -1, 0) - turn(flux, 1, 0)) * 0.5)[own]
            + (turn(side, -1, 1) - turn(side, 1, 1)) * 0.5
        )
    along_x = [((turn(f, -1, 0) - turn(f, 1, 0)) * 0.5)[own] for f in v]
    along_y = [(turn(f[own], -1, 1) - turn(f[own], 1, 1)) * 0.5 for f in v]
    direct = [
        adjoint[0][own] * along_x[0] + adjoint[1][own] * along_x[1],
        adjoint[0][own] * along_y[0] + adjoint[1][own] * along_y[1],
    ]
    for k in range(2):
        grad_velocity[k] = adjoint[k][own] - step_size * (direct[k] - cross[k]) + through[k]

    scale = factor[0, 0]
    middle1 = wide_terms(e2, 3, a1, 4, rows)
    middle0 = wide_terms(e1, 2, a0, 5, rows)

    outer = jnp.concatenate([sided(e3[c][own], 0) for c in range(2)], axis=0)
    lh, ll = halves(outer)
    ah, al = take(a2, 2, rows + 4)
    last = dot_nt(lh, ah) + dot_nt(lh, al) + dot_nt(ll, ah)
    last = last.reshape(6, rows, (rows + 4) * 32)
    group = lax.broadcasted_iota(jnp.int32, (rows, (rows + 4) * 32), 1) // 32
    line = lax.broadcasted_iota(jnp.int32, (rows, (rows + 4) * 32), 0)
    last = [
        eight_rows(
            lane_groups_summed(
                jnp.sum(jnp.where((group == line + p)[None], last, 0.0), axis=1)
            )
        )
        for p in range(3)
    ]

    inner = jnp.concatenate(
        [jnp.concatenate([turn(f, 1, 1), f, turn(f, -1, 1)], axis=0) for f in v], axis=0
    )
    lh, ll = halves(inner)
    eh0, el0 = high[32 : 32 + rows * 32], low[32 : 32 + rows * 32]
    begin = dot_nt(lh, eh0) + dot_nt(lh, el0) + dot_nt(ll, eh0)
    tall = rows + 16
    begin = begin.reshape(6, tall, rows * 32)
    group = lax.broadcasted_iota(jnp.int32, (tall, rows * 32), 1) // 32
    line = lax.broadcasted_iota(jnp.int32, (tall, rows * 32), 0)
    begin = [
        eight_rows(
            lane_groups_summed(
                jnp.sum(jnp.where((line == group + p + 7)[None], begin, 0.0), axis=1)
            )
        )
        for p in range(3)
    ]

    lane = lax.broadcasted_iota(jnp.int32, (1, 128), 1)
    ends = jnp.zeros((1, 128), F32)
    for c in range(2):
        end = jnp.sum(jnp.sum(e3[c][own], axis=0, keepdims=True), axis=1, keepdims=True)
        ends = ends + jnp.where(lane == 96 + c, end, 0.0)
    sums = [bias_line(e2, 3, rows), bias_line(e1, 2, rows), bias_line(e0, 1, rows), ends]
    sums = eight_rows(jnp.concatenate(sums, axis=0))
    kept = lax.broadcasted_iota(jnp.int32, (96, 128), 1) < 96
    rest = jnp.concatenate(last + begin + [sums, jnp.zeros((40, 128), F32)], axis=0)
    terms[0:96, :] = jnp.where(kept, middle1, rest) * scale
    terms[96:192, :] = jnp.where(kept, middle0, 0.0) * scale


def unpack_kernel(total, first, bias0, hidden, biases, last, ends):
    for p in range(3):
        for at, begin in enumerate((96, 0)):
            hidden[at, p] = total[begin : begin + 96, 32 * p : 32 * p + 32].reshape(3, 32, 32)
    rest = turn(total[0:56, :], 32, 1)[:, :32]
    for p in range(3):
        for ref, begin in ((last, 8 * p), (first, 24 + 8 * p)):
            for q in range(3):
                at = begin + q
                ref[p, q] = jnp.concatenate([rest[at : at + 1], rest[at + 3 : at + 4]], axis=0)
    biases[...] = jnp.concatenate([rest[49:50], rest[48:49]], axis=0)
    bias0[...] = rest[50:51]
    ends[...] = rest[51:52, :2]


def total_of(packed):
    lines, lanes = packed.shape
    local = (NEAR, CORE)
    part = packed.reshape(lax.axis_size(local), -1, lanes)
    part = lax.all_to_all(part, local, 0, 0, tiled=True).sum(axis=0)
    part = from_everyone(part, FAR).sum(axis=0)
    return from_everyone(part, local).reshape(lines, lanes)


def forward_taps(w):
    out, into = w.shape[2], w.shape[3]
    return jnp.transpose(w, (1, 2, 0, 3)).reshape(3 * out, 3 * into)


def backward_taps(w):
    out, into = w.shape[2], w.shape[3]
    return jnp.transpose(w[::-1, ::-1], (1, 3, 0, 2)).reshape(3 * into, 3 * out)


def narrow_taps(w):
    t = jnp.transpose(w, (2, 1, 3, 0))
    t = jnp.pad(t, ((0, 0), (0, 0), (0, 0), (0, 5))).reshape(w.shape[2], 48)
    return jnp.pad(t, ((0, 0), (0, 80)))


def out_taps_of(w):
    t = jnp.pad(w.reshape(3, 6, w.shape[3]), ((0, 0), (0, 2), (0, 0)))
    return jnp.concatenate([t] * 4, axis=2)


def flipped(w):
    return jnp.swapaxes(w[::-1, ::-1], 2, 3)


def shape_of(*dims, dtype=F32):
    return jax.ShapeDtypeStruct(dims, dtype)


def call(kernel, out_shape, scratch=(), room=63, **extra):
    return pl.pallas_call(
        kernel,
        out_shape=out_shape,
        scratch_shapes=list(scratch),
        compiler_params=pltpu.CompilerParams(vmem_limit_bytes=room * 1024 * 1024),
        **extra,
    )


def body(velocity, cotangent, w_first, b_first, w_hidden, b_hidden, w_last):
    rows, width = velocity.shape[1], velocity.shape[2]
    members = lax.axis_size(GX)
    cprev, clater = shifted(cotangent, GX, 1), shifted(cotangent, GX, -1)
    basis, sums, around = call(
        basis_kernel,
        (
            shape_of(ITERS, rows + 16, width),
            shape_of(members, 128),
            shape_of(2, rows + 16, width),
        ),
        room=16,
    )(cprev, cotangent, clater)
    gathered = lax.all_to_all(sums.reshape(members, 1, 128), GX, 0, 0, tiled=True)

    sums, w_first, b_first, w_hidden, b_hidden, w_last = lax.optimization_barrier(
        (sums, w_first, b_first, w_hidden, b_hidden, w_last)
    )
    sums, velocity = lax.optimization_barrier((sums, velocity))
    vprev, vlater = shifted(velocity, GX, 1), shifted(velocity, GX, -1)
    wide_pad = ((0, 0), (0, 256 - 96))
    wide = jnp.stack([jnp.pad(forward_taps(w_hidden[m]), wide_pad) for m in range(2)])
    wide_back = jnp.stack([jnp.pad(backward_taps(w_hidden[m]), wide_pad) for m in range(2)])
    narrow = narrow_taps(w_first)
    narrow_back = narrow_taps(flipped(w_last))
    out_taps = out_taps_of(flipped(w_first))
    biases = jnp.stack([b_first, b_hidden[0], b_hidden[1]])
    biases = jnp.broadcast_to(biases[:, :, None], (3, biases.shape[1], 128))

    heights = (rows + 10, rows + 8, rows + 6)
    held = [shape_of(h * 32, width, dtype=BF16) for h in heights for _ in range(2)]
    wide_band = shape_of(96 * BLOCK, 3 * SPAN * 32, dtype=BF16)
    narrow_band = shape_of(32 * BLOCK, 144, dtype=BF16)
    edge = -(-(rows + 2) * 32 // 128) * 128
    held += [narrow_band, wide_band, wide_band, shape_of(2, 6 * rows, edge, dtype=BF16)]
    a0h, a0l, a1h, a1l, a2h, a2l, band2, band1, band0, band_out = call(
        forward_kernel,
        tuple(held),
        [pltpu.VMEM(item.shape, item.dtype) for item in (narrow_band, wide_band, wide_band)],
    )(vprev, velocity, vlater, narrow, wide, biases, narrow_back, wide_back, out_taps)

    quick, unsafe = call(
        pressure_kernel,
        (shape_of(rows + 16, width), shape_of(1, 1, dtype=jnp.int32)),
        room=12,
        out_specs=(
            pl.BlockSpec(memory_space=pltpu.VMEM),
            pl.BlockSpec(memory_space=pltpu.SMEM),
        ),
    )(gathered.reshape(members, 128), basis)
    pressure = lax.cond(
        unsafe[0, 0] != 0,
        lambda c, _: stepwise_pressure(c),
        lambda c, q: q,
        around,
        quick,
    )

    factor = 1.0 / jnp.sqrt(jnp.float32(members * rows * width))
    whole = pl.BlockSpec(memory_space=pltpu.VMEM)
    outside = pl.BlockSpec(memory_space=pl.ANY)
    fetched = (band2, a2h, a2l, band1, a1h, a1l, band0, a0h, a0l, band_out)
    grad_velocity, terms = call(
        backward_kernel,
        (shape_of(2, rows, width), shape_of(192, 128)),
        [
            pltpu.VMEM(((rows + 6) * 32, width), F32),
            pltpu.VMEM(((rows + 4) * 32, width), F32),
            pltpu.VMEM(((rows + 2) * 32, width), F32),
            pltpu.VMEM(((rows + 6) * 32, width), BF16),
            pltpu.VMEM(((rows + 6) * 32, width), BF16),
            pltpu.VMEM(((rows + 4) * 32, width), BF16),
            pltpu.VMEM(((rows + 4) * 32, width), BF16),
        ]
        + [pltpu.VMEM(item.shape, item.dtype) for item in fetched]
        + [pltpu.SemaphoreType.DMA((len(fetched),))],
        in_specs=[pl.BlockSpec(memory_space=pltpu.SMEM)] + [whole] * 5 + [outside] * len(fetched),
    )(factor.reshape(1, 1), pressure, around, vprev, velocity, vlater, *fetched)
    total = total_of(terms)
    taps = w_first.shape[0]
    first, bias0, hidden, biases, last, ends = call(
        unpack_kernel,
        (
            shape_of(taps, taps, 2, 32),
            shape_of(1, 32),
            shape_of(2, taps, taps, 32, 32),
            shape_of(2, 32),
            shape_of(taps, taps, 2, 32),
            shape_of(1, 2),
        ),
    )(total)
    return (
        grad_velocity,
        jnp.swapaxes(first, 2, 3),
        bias0.reshape(-1),
        hidden,
        biases,
        last,
        ends.reshape(-1),
    )


def solution(mesh):
    cores, near = 2, 4
    far = mesh.shape["gx"] // (cores * near)
    finer = Mesh(mesh.devices.reshape(mesh.shape["groups"], far, near, cores), GROUPS_GX)
    placed = (P(None, GROUPS_GX, None), P(None, GROUPS_GX, None), P(), P(), P(), P(), P())
    return jax.shard_map(
        body,
        mesh=finer,
        in_specs=placed,
        out_specs=(
            P(None, GROUPS_GX, None),
            P("groups", None, None, None),
            P("groups"),
            P("groups", None, None, None, None),
            P("groups", None),
            P("groups", None, None, None),
            P("groups"),
        ),
        check_vma=False,
    )
```

```python
import jax
import jax.numpy as jnp
from jax import lax
from jax.experimental import pallas as pl
from jax.experimental.pallas import tpu as pltpu
from jax.sharding import Mesh
from jax.sharding import PartitionSpec as P


ITERS = 8
FAR, NEAR, CORE = "gx_far", "gx_near", "gx_core"
GX = (FAR, NEAR, CORE)
GROUPS_GX = ("groups", FAR, NEAR, CORE)
SPREAD_LIMIT = 3000.0
BLOCK = 6
SPAN = BLOCK + 2
F32 = jnp.float32
BF16 = jnp.bfloat16

step_size = 0.25


def from_everyone(x, axis):
    length = lax.axis_size(axis)
    return lax.all_to_all(jnp.broadcast_to(x[None], (length, *x.shape)), axis, 0, 0, tiled=True)


def shifted(value, axis, steps):
    count = lax.axis_size(axis)
    pairs = [(source, (source + steps) % count) for source in range(count)]
    return lax.ppermute(value, axis, pairs)


def turn(x, steps, axis):
    return pltpu.roll(x, steps % x.shape[axis], axis)


def halves(x):
    high = x.astype(BF16)
    return high, (x - high.astype(F32)).astype(BF16)


def starts(first, count):
    return [min(first + BLOCK * i, first + count - BLOCK) for i in range(-(-count // BLOCK))]


def fold_lanes(x):
    total = x[:, :128]
    for at in range(128, x.shape[1], 128):
        total = total + x[:, at : at + 128]
    return total


def lane_groups_summed(x):
    x = fold_lanes(x)
    x = x + turn(x, 64, 1)
    return x + turn(x, 32, 1)


def neighbours(t):
    return turn(t, 1, 0) + turn(t, -1, 0) + turn(t, 1, 1) + turn(t, -1, 1)


def basis_kernel(prev, own, later, basis, sums, around):
    rows = own.shape[1]
    first = jnp.concatenate([prev[0], own[0], later[0]], axis=0)
    second = jnp.concatenate([prev[1], own[1], later[1]], axis=0)
    source = -(turn(first, -1, 0) - first + (turn(second, -1, 1) - second))
    around[0] = first[rows - 8 : 2 * rows + 8]
    around[1] = second[rows - 8 : 2 * rows + 8]
    line = lax.broadcasted_iota(jnp.int32, (2 * ITERS, 128), 0)
    lane = lax.broadcasted_iota(jnp.int32, (2 * ITERS, 128), 1)
    squares, crosses = [], []

    def product(a, b):
        return fold_lanes(jnp.sum(a[rows : 2 * rows] * b[rows : 2 * rows], axis=0, keepdims=True))

    before, now = None, source
    for k in range(ITERS):
        basis[k] = now[rows - 8 : 2 * rows + 8]
        if k == 0:
            after = -0.25 * neighbours(now)
        else:
            after = -0.5 * neighbours(now) - before
        squares.append(product(now, now))
        crosses.append(product(now, after))
        before, now = now, after
    stacked = jnp.concatenate(squares + crosses, axis=0)
    column = jnp.sum(stacked, axis=1, keepdims=True)
    row = jnp.sum(jnp.where(line == lane, column, 0.0), axis=0, keepdims=True)
    sums[...] = jnp.broadcast_to(row, sums.shape)


def quadratic(a, b, mu):
    total = None
    for i, left in enumerate(a):
        inner = None
        for j, right in enumerate(b):
            term = right * mu[i][j]
            inner = term if inner is None else inner + term
        total = left * inner if total is None else total + left * inner
    return total


def spread(a):
    total = jnp.abs(a[0])
    for item in a[1:]:
        total = total + jnp.abs(item)
    return total


def image_of(c):
    out = [4.0 * item for item in c] + [jnp.zeros_like(c[0])]
    out[1] = out[1] + 4.0 * c[0]
    for k in range(1, len(c)):
        out[k + 1] = out[k + 1] + 2.0 * c[k]
        out[k - 1] = out[k - 1] + 2.0 * c[k]
    return out


def combined(factor, a, b):
    out = []
    for k in range(max(len(a), len(b))):
        if k >= len(a):
            out.append(b[k])
        elif k >= len(b):
            out.append(factor * a[k])
        else:
            out.append(b[k] + factor * a[k])
    return out


def pressure_kernel(gathered, basis, pressure, unsafe):
    total = jnp.sum(gathered[...], axis=0, keepdims=True)
    lane = lax.broadcasted_iota(jnp.int32, (1, 128), 1)
    items = [
        jnp.broadcast_to(jnp.sum(jnp.where(lane == k, total, 0.0), axis=1, keepdims=True), (1, 128))
        for k in range(2 * ITERS)
    ]
    moments = [items[0], items[ITERS]]
    for k in range(1, ITERS):
        moments.append(2.0 * items[k] - items[0])
        moments.append(2.0 * items[ITERS + k] - items[ITERS])
    mu = [
        [0.5 * (moments[i + j] + moments[abs(i - j)]) for j in range(min(ITERS + 1, 2 * ITERS - i))]
        for i in range(ITERS)
    ]
    one = jnp.ones((1, 128), F32)
    residual, direction, answer = [one], [one], [jnp.zeros((1, 128), F32)]
    norm_now = items[0]
    safe = norm_now > 0.0
    for step in range(ITERS):
        image = image_of(direction)
        product = quadratic(direction, image, mu)
        bound = spread(direction) * spread(image) * items[0]
        safe = safe & (product > 0.0) & (bound < SPREAD_LIMIT * product)
        alpha = norm_now / product
        answer = combined(alpha, direction, answer)
        if step + 1 < ITERS:
            residual = combined(-alpha, image, residual)
            norm_next = quadratic(residual, residual, mu)
            size = spread(residual)
            safe = safe & (norm_next > 0.0) & (size * size * items[0] < SPREAD_LIMIT * norm_next)
            direction = combined(norm_next / norm_now, direction, residual)
            norm_now = norm_next
    wide = basis.shape[2] // 128
    lam = None
    for k in range(ITERS):
        term = jnp.concatenate([answer[k]] * wide, axis=1) * basis[k]
        lam = term if lam is None else lam + term
    pressure[...] = lam
    unsafe[0, 0] = jnp.max(jnp.where(safe, 0.0, 1.0)).astype(jnp.int32)


def laplace(field):
    above = shifted(field[-1:], GX, 1)
    below = shifted(field[:1], GX, -1)
    up = jnp.concatenate([above, field[:-1]], axis=0)
    down = jnp.concatenate([field[1:], below], axis=0)
    return 4.0 * field - up - down - jnp.roll(field, 1, 1) - jnp.roll(field, -1, 1)


def sum_of(a, b):
    local = jnp.broadcast_to(jnp.sum(a * b), (1, 128))
    return jnp.sum(from_everyone(local, GX)[:, 0, 0])


def stepwise_pressure(around):
    first, second = around[0, 8:-8], around[1, 8:-8]
    below = around[0, 9:-7]
    source = -(below - first + (jnp.roll(second, -1, 1) - second))

    def iterate(_, carry):
        pressure, residual, direction, norm_now = carry
        image = laplace(direction)
        alpha = norm_now / sum_of(direction, image)
        pressure = pressure + alpha * direction
        residual = residual - alpha * image
        norm_next = sum_of(residual, residual)
        direction = residual + norm_next / norm_now * direction
        return pressure, residual, direction, norm_next

    start = (jnp.zeros_like(source), source, source, sum_of(source, source))
    pressure = lax.fori_loop(0, ITERS, iterate, start)[0]
    above = shifted(pressure[-8:], GX, 1)
    under = shifted(pressure[:8], GX, -1)
    return jnp.concatenate([above, pressure, under], axis=0)


def banded(taps):
    rows = jnp.concatenate([taps] + [turn(taps, 32 * r, 1) for r in range(1, BLOCK)], axis=0)
    high, low = halves(rows)
    return jnp.concatenate([high, high, low], axis=1)


def banded_narrow(taps):
    rows = jnp.concatenate([taps] + [turn(taps, r, 1) for r in range(1, BLOCK)], axis=0)
    high, low = halves(rows)
    return jnp.concatenate([high[:, :48], high[:, :48], low[:, :48]], axis=1)


def banded_out(taps, rows):
    width = (rows + 2) * 32
    padded = -(-width // 128)
    lane = lax.broadcasted_iota(jnp.int32, (rows, padded * 128), 1) // 32
    row = lax.broadcasted_iota(jnp.int32, (rows, padded * 128), 0)
    pieces = []
    for j in range(6):
        piece = jnp.zeros((rows, padded * 128), F32)
        for p in range(3):
            line = jnp.concatenate([taps[p][j : j + 1]] * padded, axis=1)
            piece = piece + jnp.where(lane == row + p, line, 0.0)
        pieces.append(piece)
    return halves(jnp.concatenate(pieces, axis=0))


def side_sum(y):
    n = y.shape[1] // 3
    return turn(y[:, :n], 1, 2) + y[:, n : 2 * n] + turn(y[:, 2 * n :], -1, 2)


def wide_conv(weights, high, low):
    x = jnp.concatenate([high, low, high], axis=0)
    y = jnp.dot(weights, x, preferred_element_type=F32)
    return side_sum(y.reshape(BLOCK, 96, y.shape[1]))


def narrow_conv(weights, pair):
    x = jnp.concatenate(pair, axis=0)
    high, low = halves(jnp.concatenate([turn(x, 1, 1), x, turn(x, -1, 1)], axis=0))
    x = jnp.concatenate([high, low, high], axis=0)
    y = jnp.dot(weights, x, preferred_element_type=F32)
    return y.reshape(BLOCK, 32, y.shape[1])


def rows_at(at, rows):
    return pl.ds(at * 32 if isinstance(at, int) else pl.multiple_of(at * 32, 32), rows * 32)


def each_block(first, count, visit):
    def step(i, _):
        visit(first + jnp.minimum(BLOCK * i, count - BLOCK))
        return 0

    lax.fori_loop(0, -(-count // BLOCK), step, 0)


def put(refs, at, value):
    high, low = halves(value.reshape(value.shape[0] * 32, value.shape[2]))
    span = rows_at(at, value.shape[0])
    refs[0][span, :] = high
    refs[1][span, :] = low


def take(refs, at, rows):
    span = rows_at(at, rows)
    return refs[0][span, :], refs[1][span, :]


def forward_kernel(
    prev,
    own,
    later,
    narrow,
    wide,
    bias,
    narrow_back,
    wide_back,
    out_taps,
    a0h,
    a0l,
    a1h,
    a1l,
    a2h,
    a2l,
    band2,
    band1,
    band0,
    band_out,
    weights0,
    weights1,
    weights2,
):
    rows, width = own.shape[1], own.shape[2]
    v = [jnp.concatenate([prev[c, rows - 8 :], own[c], later[c, :8]], axis=0) for c in range(2)]
    weights0[...] = banded_narrow(narrow[...])
    weights1[...] = banded(wide[0])
    weights2[...] = banded(wide[1])
    shift = [jnp.concatenate([bias[m]] * (width // 128), axis=1) for m in range(3)]
    for s in starts(-5, rows + 10):
        pair = [v[c][s + 7 : s + 7 + SPAN] for c in range(2)]
        put((a0h, a0l), s + 5, jnp.tanh(narrow_conv(weights0[...], pair) + shift[0]))
    for s in starts(-4, rows + 8):
        x = take((a0h, a0l), s + 4, SPAN)
        put((a1h, a1l), s + 4, jnp.tanh(wide_conv(weights1[...], *x) + shift[1]))
    for s in starts(-3, rows + 6):
        x = take((a1h, a1l), s + 3, SPAN)
        put((a2h, a2l), s + 3, jnp.tanh(wide_conv(weights2[...], *x) + shift[2]))
    band2[...] = banded_narrow(narrow_back[...])
    band1[...] = banded(wide_back[1])
    band0[...] = banded(wide_back[0])
    high, low = banded_out(out_taps[...], rows)
    band_out[0] = high
    band_out[1] = low


def dot_nt(a, b):
    return lax.dot_general(a, b, (((1,), (1,)), ((), ())), preferred_element_type=F32)


def sided(e, axis):
    return jnp.concatenate([turn(e, -1, e.ndim - 1), e, turn(e, 1, e.ndim - 1)], axis=axis)


def wide_terms(err, err_at, act, act_at, rows, held):
    held[...] = jnp.zeros_like(held)

    def step(i, _):
        s = jnp.minimum(BLOCK * i, rows - BLOCK)
        e = err[rows_at(err_at + s, BLOCK), :].reshape(BLOCK, 32, -1)
        line = lax.broadcasted_iota(jnp.int32, e.shape, 0)
        e = jnp.where(line >= BLOCK * i - s, e, 0.0)
        high, low = halves(sided(e, 1).reshape(BLOCK * 96, -1))
        ah, al = take(act, act_at + s - 1, SPAN)
        held[...] += dot_nt(
            jnp.concatenate([high, high, low], axis=1), jnp.concatenate([ah, al, ah], axis=1)
        )
        return 0

    lax.fori_loop(0, -(-rows // BLOCK), step, 0)
    total = held[...]
    total = total.reshape(BLOCK, 96, SPAN * 32)
    out = None
    for r in range(BLOCK):
        piece = turn(total[r], -32 * r, 1)[:, :128]
        out = piece if out is None else out + piece
    return out


def eight_rows(x):
    missing = 8 - x.shape[0]
    if not missing:
        return x
    return jnp.concatenate([x, jnp.zeros((missing, x.shape[1]), x.dtype)], axis=0)


def bias_line(err, err_at, rows):
    e = err[pl.ds(err_at * 32, rows * 32), :].reshape(rows, 32, -1)
    column = jnp.sum(fold_lanes(jnp.sum(e, axis=0)), axis=1, keepdims=True)
    line = lax.broadcasted_iota(jnp.int32, (32, 128), 0)
    lane = lax.broadcasted_iota(jnp.int32, (32, 128), 1)
    return jnp.sum(jnp.where(lane == line + 96, column, 0.0), axis=0, keepdims=True)


def backward_kernel(
    factor,
    pressure,
    around,
    vprev,
    vown,
    vlater,
    far2,
    far2h,
    far2l,
    far1,
    far1h,
    far1l,
    far0,
    far0h,
    far0l,
    far_out,
    grad_velocity,
    terms,
    e2,
    e1,
    e0,
    eh,
    el,
    fh,
    fl,
    held,
    band2,
    a2h,
    a2l,
    band1,
    a1h,
    a1l,
    band0,
    a0h,
    a0l,
    band_out,
    arrived,
):
    rows, width = vown.shape[1], vown.shape[2]
    a0, a1, a2, split = (a0h, a0l), (a1h, a1l), (a2h, a2l), (eh, el)
    other = (fh, fl)
    sources = (far2, far2h, far2l, far1, far1h, far1l, far0, far0h, far0l, far_out)
    targets = (band2, a2h, a2l, band1, a1h, a1l, band0, a0h, a0l, band_out)
    copies = [
        pltpu.make_async_copy(source, target, arrived.at[i])
        for i, (source, target) in enumerate(zip(sources, targets))
    ]
    for copy in copies:
        copy.start()

    lam = pressure[...]
    adjoint = [around[0] - (lam - turn(lam, 1, 0)), around[1] - (lam - turn(lam, 1, 1))]
    v = [jnp.concatenate([vprev[c, rows - 8 :], vown[c], vlater[c, :8]], axis=0) for c in range(2)]
    e3 = [step_size * item for item in adjoint]

    def slope_of(act, at):
        high, low = take(act, at, BLOCK)
        a = high.astype(F32) + low.astype(F32)
        return (1.0 - a * a).reshape(BLOCK, 32, width)

    def keep(ref, parts, at, value):
        put(parts, at, value)
        ref[rows_at(at, BLOCK), :] = value.reshape(BLOCK * 32, width)

    for copy in copies[:3]:
        copy.wait()
    for s in starts(-3, rows + 6):
        pair = [e3[c][s + 7 : s + 7 + SPAN] for c in range(2)]
        keep(e2, split, s + 3, narrow_conv(band2[...], pair) * slope_of(a2, s + 3))
    for copy in copies[3:6]:
        copy.wait()

    def middle(s):
        x = take(split, s + 2, SPAN)
        keep(e1, other, s + 2, wide_conv(band1[...], *x) * slope_of(a1, s + 4))

    each_block(-2, rows + 4, middle)
    for copy in copies[6:]:
        copy.wait()

    def foremost(s):
        x = take(other, s + 1, SPAN)
        keep(e0, split, s + 1, wide_conv(band0[...], *x) * slope_of(a0, s + 5))

    each_block(-1, rows + 2, foremost)

    own = slice(8, 8 + rows)
    cells = (rows + 2) * 32
    high, low = eh[0:cells, :], el[0:cells, :]
    wh, wl = band_out[0, :, :cells], band_out[1, :, :cells]
    y = (
        jnp.dot(wh, high, preferred_element_type=F32)
        + jnp.dot(wh, low, preferred_element_type=F32)
        + jnp.dot(wl, high, preferred_element_type=F32)
    )
    through = []
    for c in range(2):
        parts = [y[(2 * q + c) * rows : (2 * q + c + 1) * rows] for q in range(3)]
        through.append(turn(parts[0], 1, 1) + parts[1] + turn(parts[2], -1, 1))

    cross = []
    for k in range(2):
        flux = v[0] * adjoint[k]
        side = v[1][own] * adjoint[k][own]
        cross.append(
            ((turn(flux, -1, 0) - turn(flux, 1, 0)) * 0.5)[own]
            + (turn(side, -1, 1) - turn(side, 1, 1)) * 0.5
        )
    along_x = [((turn(f, -1, 0) - turn(f, 1, 0)) * 0.5)[own] for f in v]
    along_y = [(turn(f[own], -1, 1) - turn(f[own], 1, 1)) * 0.5 for f in v]
    direct = [
        adjoint[0][own] * along_x[0] + adjoint[1][own] * along_x[1],
        adjoint[0][own] * along_y[0] + adjoint[1][own] * along_y[1],
    ]
    for k in range(2):
        grad_velocity[k] = adjoint[k][own] - step_size * (direct[k] - cross[k]) + through[k]

    scale = factor[0, 0]
    middle1 = wide_terms(e2, 3, a1, 4, rows, held)
    middle0 = wide_terms(e1, 2, a0, 5, rows, held)

    outer = jnp.concatenate([sided(e3[c][own], 0) for c in range(2)], axis=0)
    lh, ll = halves(outer)
    ah, al = take(a2, 2, rows + 4)
    last = dot_nt(lh, ah) + dot_nt(lh, al) + dot_nt(ll, ah)
    last = last.reshape(6, rows, (rows + 4) * 32)
    group = lax.broadcasted_iota(jnp.int32, (rows, (rows + 4) * 32), 1) // 32
    line = lax.broadcasted_iota(jnp.int32, (rows, (rows + 4) * 32), 0)
    last = [
        eight_rows(
            lane_groups_summed(
                jnp.sum(jnp.where((group == line + p)[None], last, 0.0), axis=1)
            )
        )
        for p in range(3)
    ]

    inner = jnp.concatenate(
        [jnp.concatenate([turn(f, 1, 1), f, turn(f, -1, 1)], axis=0) for f in v], axis=0
    )
    lh, ll = halves(inner)
    eh0, el0 = high[32 : 32 + rows * 32], low[32 : 32 + rows * 32]
    begin = dot_nt(lh, eh0) + dot_nt(lh, el0) + dot_nt(ll, eh0)
    tall = rows + 16
    begin = begin.reshape(6, tall, rows * 32)
    group = lax.broadcasted_iota(jnp.int32, (tall, rows * 32), 1) // 32
    line = lax.broadcasted_iota(jnp.int32, (tall, rows * 32), 0)
    begin = [
        eight_rows(
            lane_groups_summed(
                jnp.sum(jnp.where((line == group + p + 7)[None], begin, 0.0), axis=1)
            )
        )
        for p in range(3)
    ]

    lane = lax.broadcasted_iota(jnp.int32, (1, 128), 1)
    ends = jnp.zeros((1, 128), F32)
    for c in range(2):
        end = jnp.sum(jnp.sum(e3[c][own], axis=0, keepdims=True), axis=1, keepdims=True)
        ends = ends + jnp.where(lane == 96 + c, end, 0.0)
    sums = [bias_line(e2, 3, rows), bias_line(e1, 2, rows), bias_line(e0, 1, rows), ends]
    sums = eight_rows(jnp.concatenate(sums, axis=0))
    kept = lax.broadcasted_iota(jnp.int32, (96, 128), 1) < 96
    rest = jnp.concatenate(last + begin + [sums, jnp.zeros((40, 128), F32)], axis=0)
    terms[0:96, :] = jnp.where(kept, middle1, rest) * scale
    terms[96:192, :] = jnp.where(kept, middle0, 0.0) * scale


def unpack_kernel(total, first, bias0, hidden, biases, last, ends):
    for p in range(3):
        for at, begin in enumerate((96, 0)):
            hidden[at, p] = total[begin : begin + 96, 32 * p : 32 * p + 32].reshape(3, 32, 32)
    rest = turn(total[0:56, :], 32, 1)[:, :32]
    for p in range(3):
        for ref, begin in ((last, 8 * p), (first, 24 + 8 * p)):
            for q in range(3):
                at = begin + q
                ref[p, q] = jnp.concatenate([rest[at : at + 1], rest[at + 3 : at + 4]], axis=0)
    biases[...] = jnp.concatenate([rest[49:50], rest[48:49]], axis=0)
    bias0[...] = rest[50:51]
    ends[...] = rest[51:52, :2]


def total_of(packed):
    lines, lanes = packed.shape
    local = (NEAR, CORE)
    part = packed.reshape(lax.axis_size(local), -1, lanes)
    part = lax.all_to_all(part, local, 0, 0, tiled=True).sum(axis=0)
    part = from_everyone(part, FAR).sum(axis=0)
    return from_everyone(part, local).reshape(lines, lanes)


def forward_taps(w):
    out, into = w.shape[2], w.shape[3]
    return jnp.transpose(w, (1, 2, 0, 3)).reshape(3 * out, 3 * into)


def backward_taps(w):
    out, into = w.shape[2], w.shape[3]
    return jnp.transpose(w[::-1, ::-1], (1, 3, 0, 2)).reshape(3 * into, 3 * out)


def narrow_taps(w):
    t = jnp.transpose(w, (2, 1, 3, 0))
    t = jnp.pad(t, ((0, 0), (0, 0), (0, 0), (0, 5))).reshape(w.shape[2], 48)
    return jnp.pad(t, ((0, 0), (0, 80)))


def out_taps_of(w):
    t = jnp.pad(w.reshape(3, 6, w.shape[3]), ((0, 0), (0, 2), (0, 0)))
    return jnp.concatenate([t] * 4, axis=2)


def flipped(w):
    return jnp.swapaxes(w[::-1, ::-1], 2, 3)


def shape_of(*dims, dtype=F32):
    return jax.ShapeDtypeStruct(dims, dtype)


def call(kernel, out_shape, scratch=(), room=63, **extra):
    return pl.pallas_call(
        kernel,
        out_shape=out_shape,
        scratch_shapes=list(scratch),
        compiler_params=pltpu.CompilerParams(vmem_limit_bytes=room * 1024 * 1024),
        **extra,
    )


def body(velocity, cotangent, w_first, b_first, w_hidden, b_hidden, w_last):
    rows, width = velocity.shape[1], velocity.shape[2]
    members = lax.axis_size(GX)
    cprev, clater = shifted(cotangent, GX, 1), shifted(cotangent, GX, -1)
    basis, sums, around = call(
        basis_kernel,
        (
            shape_of(ITERS, rows + 16, width),
            shape_of(members, 128),
            shape_of(2, rows + 16, width),
        ),
        room=16,
    )(cprev, cotangent, clater)
    gathered = lax.all_to_all(sums.reshape(members, 1, 128), GX, 0, 0, tiled=True)

    sums, w_first, b_first, w_hidden, b_hidden, w_last = lax.optimization_barrier(
        (sums, w_first, b_first, w_hidden, b_hidden, w_last)
    )
    sums, velocity = lax.optimization_barrier((sums, velocity))
    vprev, vlater = shifted(velocity, GX, 1), shifted(velocity, GX, -1)
    wide_pad = ((0, 0), (0, 256 - 96))
    wide = jnp.stack([jnp.pad(forward_taps(w_hidden[m]), wide_pad) for m in range(2)])
    wide_back = jnp.stack([jnp.pad(backward_taps(w_hidden[m]), wide_pad) for m in range(2)])
    narrow = narrow_taps(w_first)
    narrow_back = narrow_taps(flipped(w_last))
    out_taps = out_taps_of(flipped(w_first))
    biases = jnp.stack([b_first, b_hidden[0], b_hidden[1]])
    biases = jnp.broadcast_to(biases[:, :, None], (3, biases.shape[1], 128))

    heights = (rows + 10, rows + 8, rows + 6)
    held = [shape_of(h * 32, width, dtype=BF16) for h in heights for _ in range(2)]
    wide_band = shape_of(96 * BLOCK, 3 * SPAN * 32, dtype=BF16)
    narrow_band = shape_of(32 * BLOCK, 144, dtype=BF16)
    edge = -(-(rows + 2) * 32 // 128) * 128
    held += [narrow_band, wide_band, wide_band, shape_of(2, 6 * rows, edge, dtype=BF16)]
    a0h, a0l, a1h, a1l, a2h, a2l, band2, band1, band0, band_out = call(
        forward_kernel,
        tuple(held),
        [pltpu.VMEM(item.shape, item.dtype) for item in (narrow_band, wide_band, wide_band)],
    )(vprev, velocity, vlater, narrow, wide, biases, narrow_back, wide_back, out_taps)

    quick, unsafe = call(
        pressure_kernel,
        (shape_of(rows + 16, width), shape_of(1, 1, dtype=jnp.int32)),
        room=12,
        out_specs=(
            pl.BlockSpec(memory_space=pltpu.VMEM),
            pl.BlockSpec(memory_space=pltpu.SMEM),
        ),
    )(gathered.reshape(members, 128), basis)
    pressure = lax.cond(
        unsafe[0, 0] != 0,
        lambda c, _: stepwise_pressure(c),
        lambda c, q: q,
        around,
        quick,
    )

    factor = 1.0 / jnp.sqrt(jnp.float32(members * rows * width))
    whole = pl.BlockSpec(memory_space=pltpu.VMEM)
    outside = pl.BlockSpec(memory_space=pl.ANY)
    fetched = (band2, a2h, a2l, band1, a1h, a1l, band0, a0h, a0l, band_out)
    grad_velocity, terms = call(
        backward_kernel,
        (shape_of(2, rows, width), shape_of(192, 128)),
        [
            pltpu.VMEM(((rows + 6) * 32, width), F32),
            pltpu.VMEM(((rows + 4) * 32, width), F32),
            pltpu.VMEM(((rows + 2) * 32, width), F32),
            pltpu.VMEM(((rows + 6) * 32, width), BF16),
            pltpu.VMEM(((rows + 6) * 32, width), BF16),
            pltpu.VMEM(((rows + 4) * 32, width), BF16),
            pltpu.VMEM(((rows + 4) * 32, width), BF16),
            pltpu.VMEM((BLOCK * 96, SPAN * 32), F32),
        ]
        + [pltpu.VMEM(item.shape, item.dtype) for item in fetched]
        + [pltpu.SemaphoreType.DMA((len(fetched),))],
        in_specs=[pl.BlockSpec(memory_space=pltpu.SMEM)] + [whole] * 5 + [outside] * len(fetched),
    )(factor.reshape(1, 1), pressure, around, vprev, velocity, vlater, *fetched)
    total = total_of(terms)
    taps = w_first.shape[0]
    first, bias0, hidden, biases, last, ends = call(
        unpack_kernel,
        (
            shape_of(taps, taps, 2, 32),
            shape_of(1, 32),
            shape_of(2, taps, taps, 32, 32),
            shape_of(2, 32),
            shape_of(taps, taps, 2, 32),
            shape_of(1, 2),
        ),
    )(total)
    return (
        grad_velocity,
        jnp.swapaxes(first, 2, 3),
        bias0.reshape(-1),
        hidden,
        biases,
        last,
        ends.reshape(-1),
    )


def solution(mesh):
    cores, near = 2, 4
    far = mesh.shape["gx"] // (cores * near)
    finer = Mesh(mesh.devices.reshape(mesh.shape["groups"], far, near, cores), GROUPS_GX)
    placed = (P(None, GROUPS_GX, None), P(None, GROUPS_GX, None), P(), P(), P(), P(), P())
    return jax.shard_map(
        body,
        mesh=finer,
        in_specs=placed,
        out_specs=(
            P(None, GROUPS_GX, None),
            P("groups", None, None, None),
            P("groups"),
            P("groups", None, None, None, None),
            P("groups", None),
            P("groups", None, None, None),
            P("groups"),
        ),
        check_vma=False,
    )
```

```python
import jax
import jax.numpy as jnp
from jax import lax
from jax.experimental import pallas as pl
from jax.experimental.pallas import tpu as pltpu
from jax.sharding import Mesh
from jax.sharding import PartitionSpec as P


ITERS = 8
FAR, NEAR, CORE = "gx_far", "gx_near", "gx_core"
GX = (FAR, NEAR, CORE)
GROUPS_GX = ("groups", FAR, NEAR, CORE)
SPREAD_LIMIT = 3000.0
BLOCK = 6
SPAN = BLOCK + 2
F32 = jnp.float32
BF16 = jnp.bfloat16

step_size = 0.25


def from_everyone(x, axis):
    length = lax.axis_size(axis)
    return lax.all_to_all(jnp.broadcast_to(x[None], (length, *x.shape)), axis, 0, 0, tiled=True)


def shifted(value, axis, steps):
    count = lax.axis_size(axis)
    pairs = [(source, (source + steps) % count) for source in range(count)]
    return lax.ppermute(value, axis, pairs)


def turn(x, steps, axis):
    return pltpu.roll(x, steps % x.shape[axis], axis)


def halves(x):
    high = x.astype(BF16)
    return high, (x - high.astype(F32)).astype(BF16)


def starts(first, count):
    return [min(first + BLOCK * i, first + count - BLOCK) for i in range(-(-count // BLOCK))]


def blocks(first, count):
    return [(s, first + BLOCK * i - s) for i, s in enumerate(starts(first, count))]


def fold_lanes(x):
    total = x[:, :128]
    for at in range(128, x.shape[1], 128):
        total = total + x[:, at : at + 128]
    return total


def lane_groups_summed(x):
    x = fold_lanes(x)
    x = x + turn(x, 64, 1)
    return x + turn(x, 32, 1)


def neighbours(t):
    return turn(t, 1, 0) + turn(t, -1, 0) + turn(t, 1, 1) + turn(t, -1, 1)


def basis_kernel(prev, own, later, basis, sums, around):
    rows = own.shape[1]
    first = jnp.concatenate([prev[0], own[0], later[0]], axis=0)
    second = jnp.concatenate([prev[1], own[1], later[1]], axis=0)
    source = -(turn(first, -1, 0) - first + (turn(second, -1, 1) - second))
    around[0] = first[rows - 8 : 2 * rows + 8]
    around[1] = second[rows - 8 : 2 * rows + 8]
    line = lax.broadcasted_iota(jnp.int32, (2 * ITERS, 128), 0)
    lane = lax.broadcasted_iota(jnp.int32, (2 * ITERS, 128), 1)
    squares, crosses = [], []

    def product(a, b):
        return fold_lanes(jnp.sum(a[rows : 2 * rows] * b[rows : 2 * rows], axis=0, keepdims=True))

    before, now = None, source
    for k in range(ITERS):
        basis[k] = now[rows - 8 : 2 * rows + 8]
        if k == 0:
            after = -0.25 * neighbours(now)
        else:
            after = -0.5 * neighbours(now) - before
        squares.append(product(now, now))
        crosses.append(product(now, after))
        before, now = now, after
    stacked = jnp.concatenate(squares + crosses, axis=0)
    column = jnp.sum(stacked, axis=1, keepdims=True)
    row = jnp.sum(jnp.where(line == lane, column, 0.0), axis=0, keepdims=True)
    sums[...] = jnp.broadcast_to(row, sums.shape)


def quadratic(a, b, mu):
    total = None
    for i, left in enumerate(a):
        inner = None
        for j, right in enumerate(b):
            term = right * mu[i][j]
            inner = term if inner is None else inner + term
        total = left * inner if total is None else total + left * inner
    return total


def spread(a):
    total = jnp.abs(a[0])
    for item in a[1:]:
        total = total + jnp.abs(item)
    return total


def image_of(c):
    out = [4.0 * item for item in c] + [jnp.zeros_like(c[0])]
    out[1] = out[1] + 4.0 * c[0]
    for k in range(1, len(c)):
        out[k + 1] = out[k + 1] + 2.0 * c[k]
        out[k - 1] = out[k - 1] + 2.0 * c[k]
    return out


def combined(factor, a, b):
    out = []
    for k in range(max(len(a), len(b))):
        if k >= len(a):
            out.append(b[k])
        elif k >= len(b):
            out.append(factor * a[k])
        else:
            out.append(b[k] + factor * a[k])
    return out


def pressure_kernel(gathered, basis, pressure, unsafe):
    total = jnp.sum(gathered[...], axis=0, keepdims=True)
    lane = lax.broadcasted_iota(jnp.int32, (1, 128), 1)
    items = [
        jnp.broadcast_to(jnp.sum(jnp.where(lane == k, total, 0.0), axis=1, keepdims=True), (1, 128))
        for k in range(2 * ITERS)
    ]
    moments = [items[0], items[ITERS]]
    for k in range(1, ITERS):
        moments.append(2.0 * items[k] - items[0])
        moments.append(2.0 * items[ITERS + k] - items[ITERS])
    mu = [
        [0.5 * (moments[i + j] + moments[abs(i - j)]) for j in range(min(ITERS + 1, 2 * ITERS - i))]
        for i in range(ITERS)
    ]
    one = jnp.ones((1, 128), F32)
    residual, direction, answer = [one], [one], [jnp.zeros((1, 128), F32)]
    norm_now = items[0]
    safe = norm_now > 0.0
    for step in range(ITERS):
        image = image_of(direction)
        product = quadratic(direction, image, mu)
        bound = spread(direction) * spread(image) * items[0]
        safe = safe & (product > 0.0) & (bound < SPREAD_LIMIT * product)
        alpha = norm_now / product
        answer = combined(alpha, direction, answer)
        if step + 1 < ITERS:
            residual = combined(-alpha, image, residual)
            norm_next = quadratic(residual, residual, mu)
            size = spread(residual)
            safe = safe & (norm_next > 0.0) & (size * size * items[0] < SPREAD_LIMIT * norm_next)
            direction = combined(norm_next / norm_now, direction, residual)
            norm_now = norm_next
    wide = basis.shape[2] // 128
    lam = None
    for k in range(ITERS):
        term = jnp.concatenate([answer[k]] * wide, axis=1) * basis[k]
        lam = term if lam is None else lam + term
    pressure[...] = lam
    unsafe[0, 0] = jnp.max(jnp.where(safe, 0.0, 1.0)).astype(jnp.int32)


def laplace(field):
    above = shifted(field[-1:], GX, 1)
    below = shifted(field[:1], GX, -1)
    up = jnp.concatenate([above, field[:-1]], axis=0)
    down = jnp.concatenate([field[1:], below], axis=0)
    return 4.0 * field - up - down - jnp.roll(field, 1, 1) - jnp.roll(field, -1, 1)


def sum_of(a, b):
    local = jnp.broadcast_to(jnp.sum(a * b), (1, 128))
    return jnp.sum(from_everyone(local, GX)[:, 0, 0])


def stepwise_pressure(around):
    first, second = around[0, 8:-8], around[1, 8:-8]
    below = around[0, 9:-7]
    source = -(below - first + (jnp.roll(second, -1, 1) - second))

    def iterate(_, carry):
        pressure, residual, direction, norm_now = carry
        image = laplace(direction)
        alpha = norm_now / sum_of(direction, image)
        pressure = pressure + alpha * direction
        residual = residual - alpha * image
        norm_next = sum_of(residual, residual)
        direction = residual + norm_next / norm_now * direction
        return pressure, residual, direction, norm_next

    start = (jnp.zeros_like(source), source, source, sum_of(source, source))
    pressure = lax.fori_loop(0, ITERS, iterate, start)[0]
    above = shifted(pressure[-8:], GX, 1)
    under = shifted(pressure[:8], GX, -1)
    return jnp.concatenate([above, pressure, under], axis=0)


def banded(taps):
    rows = jnp.concatenate([taps] + [turn(taps, 32 * r, 1) for r in range(1, BLOCK)], axis=0)
    high, low = halves(rows)
    return jnp.concatenate([high, high, low], axis=1)


def banded_narrow(taps):
    rows = jnp.concatenate([taps] + [turn(taps, r, 1) for r in range(1, BLOCK)], axis=0)
    high, low = halves(rows)
    return jnp.concatenate([high[:, :48], high[:, :48], low[:, :48]], axis=1)


def banded_out(taps, rows):
    width = (rows + 2) * 32
    padded = -(-width // 128)
    lane = lax.broadcasted_iota(jnp.int32, (rows, padded * 128), 1) // 32
    row = lax.broadcasted_iota(jnp.int32, (rows, padded * 128), 0)
    pieces = []
    for j in range(6):
        piece = jnp.zeros((rows, padded * 128), F32)
        for p in range(3):
            line = jnp.concatenate([taps[p][j : j + 1]] * padded, axis=1)
            piece = piece + jnp.where(lane == row + p, line, 0.0)
        pieces.append(piece)
    return halves(jnp.concatenate(pieces, axis=0))


def side_sum(y):
    n = y.shape[1] // 3
    return turn(y[:, :n], 1, 2) + y[:, n : 2 * n] + turn(y[:, 2 * n :], -1, 2)


def wide_conv(weights, high, low):
    x = jnp.concatenate([high, low, high], axis=0)
    y = jnp.dot(weights, x, preferred_element_type=F32)
    return side_sum(y.reshape(-1, 96, y.shape[1]))


def narrow_conv(weights, pair):
    x = jnp.concatenate(pair, axis=0)
    high, low = halves(jnp.concatenate([turn(x, 1, 1), x, turn(x, -1, 1)], axis=0))
    x = jnp.concatenate([high, low, high], axis=0)
    y = jnp.dot(weights, x, preferred_element_type=F32)
    return y.reshape(-1, 32, y.shape[1])


def put(refs, at, value):
    high, low = halves(value.reshape(value.shape[0] * 32, value.shape[2]))
    span = pl.ds(at * 32, value.shape[0] * 32)
    refs[0][span, :] = high
    refs[1][span, :] = low


def take(refs, at, rows):
    span = pl.ds(at * 32, rows * 32)
    return refs[0][span, :], refs[1][span, :]


def forward_kernel(
    prev,
    own,
    later,
    narrow,
    wide,
    bias,
    narrow_back,
    wide_back,
    out_taps,
    a0h,
    a0l,
    a1h,
    a1l,
    a2h,
    a2l,
    band2,
    band1,
    band0,
    band_out,
    weights0,
    weights1,
    weights2,
):
    rows, width = own.shape[1], own.shape[2]
    v = [jnp.concatenate([prev[c, rows - 8 :], own[c], later[c, :8]], axis=0) for c in range(2)]
    weights0[...] = banded_narrow(narrow[...])
    weights1[...] = banded(wide[0])
    weights2[...] = banded(wide[1])
    shift = [jnp.concatenate([bias[m]] * (width // 128), axis=1) for m in range(3)]
    for s in starts(-5, rows + 10):
        pair = [v[c][s + 7 : s + 7 + SPAN] for c in range(2)]
        put((a0h, a0l), s + 5, jnp.tanh(narrow_conv(weights0[...], pair) + shift[0]))
    for s in starts(-4, rows + 8):
        x = take((a0h, a0l), s + 4, SPAN)
        put((a1h, a1l), s + 4, jnp.tanh(wide_conv(weights1[...], *x) + shift[1]))
    for s in starts(-3, rows + 6):
        x = take((a1h, a1l), s + 3, SPAN)
        put((a2h, a2l), s + 3, jnp.tanh(wide_conv(weights2[...], *x) + shift[2]))
    band2[...] = banded_narrow(narrow_back[...])
    band1[...] = banded(wide_back[1])
    band0[...] = banded(wide_back[0])
    high, low = banded_out(out_taps[...], rows)
    band_out[0] = high
    band_out[1] = low


def dot_nt(a, b):
    return lax.dot_general(a, b, (((1,), (1,)), ((), ())), preferred_element_type=F32)


def sided(e, axis):
    return jnp.concatenate([turn(e, -1, e.ndim - 1), e, turn(e, 1, e.ndim - 1)], axis=axis)


def wide_terms(err, err_at, act, act_at, rows):
    total = None
    for s, done in blocks(0, rows):
        e = err[pl.ds((err_at + s + done) * 32, (BLOCK - done) * 32), :]
        e = e.reshape(BLOCK - done, 32, -1)
        high, low = halves(sided(e, 1).reshape((BLOCK - done) * 96, -1))
        ah, al = take(act, act_at + s - 1, SPAN)
        term = dot_nt(
            jnp.concatenate([high, high, low], axis=1), jnp.concatenate([ah, al, ah], axis=1)
        )
        if done:
            term = jnp.concatenate([total[: 96 * done], total[96 * done :] + term], axis=0)
            total = term
        else:
            total = term if total is None else total + term
    total = total.reshape(BLOCK, 96, SPAN * 32)
    out = None
    for r in range(BLOCK):
        piece = turn(total[r], -32 * r, 1)[:, :128]
        out = piece if out is None else out + piece
    return out


def eight_rows(x):
    missing = 8 - x.shape[0]
    if not missing:
        return x
    return jnp.concatenate([x, jnp.zeros((missing, x.shape[1]), x.dtype)], axis=0)


def bias_line(err, err_at, rows):
    e = err[pl.ds(err_at * 32, rows * 32), :].reshape(rows, 32, -1)
    column = jnp.sum(fold_lanes(jnp.sum(e, axis=0)), axis=1, keepdims=True)
    line = lax.broadcasted_iota(jnp.int32, (32, 128), 0)
    lane = lax.broadcasted_iota(jnp.int32, (32, 128), 1)
    return jnp.sum(jnp.where(lane == line + 96, column, 0.0), axis=0, keepdims=True)


def backward_kernel(
    factor,
    pressure,
    around,
    vprev,
    vown,
    vlater,
    far2,
    far2h,
    far2l,
    far1,
    far1h,
    far1l,
    far0,
    far0h,
    far0l,
    far_out,
    grad_velocity,
    terms,
    e2,
    e1,
    e0,
    eh,
    el,
    fh,
    fl,
    band2,
    a2h,
    a2l,
    band1,
    a1h,
    a1l,
    band0,
    a0h,
    a0l,
    band_out,
    arrived,
):
    rows, width = vown.shape[1], vown.shape[2]
    a0, a1, a2, split = (a0h, a0l), (a1h, a1l), (a2h, a2l), (eh, el)
    other = (fh, fl)
    sources = (far2, far2h, far2l, far1, far1h, far1l, far0, far0h, far0l, far_out)
    targets = (band2, a2h, a2l, band1, a1h, a1l, band0, a0h, a0l, band_out)
    copies = [
        pltpu.make_async_copy(source, target, arrived.at[i])
        for i, (source, target) in enumerate(zip(sources, targets))
    ]
    for copy in copies:
        copy.start()

    lam = pressure[...]
    adjoint = [around[0] - (lam - turn(lam, 1, 0)), around[1] - (lam - turn(lam, 1, 1))]
    v = [jnp.concatenate([vprev[c, rows - 8 :], vown[c], vlater[c, :8]], axis=0) for c in range(2)]
    e3 = [step_size * item for item in adjoint]

    def slope_of(act, at, count):
        high, low = take(act, at, count)
        a = high.astype(F32) + low.astype(F32)
        return (1.0 - a * a).reshape(count, 32, width)

    def keep(ref, parts, at, value):
        put(parts, at, value)
        ref[pl.ds(at * 32, value.shape[0] * 32), :] = value.reshape(value.shape[0] * 32, width)

    for copy in copies[:3]:
        copy.wait()
    for s, done in blocks(-3, rows + 6):
        pair = [e3[c][s + 7 : s + 7 + SPAN] for c in range(2)]
        slope = slope_of(a2, s + 3 + done, BLOCK - done)
        keep(e2, split, s + 3 + done, narrow_conv(band2[32 * done :, :], pair) * slope)
    for copy in copies[3:6]:
        copy.wait()
    for s, done in blocks(-2, rows + 4):
        x = take(split, s + 2, SPAN)
        slope = slope_of(a1, s + 4 + done, BLOCK - done)
        keep(e1, other, s + 2 + done, wide_conv(band1[96 * done :, :], *x) * slope)
    for copy in copies[6:]:
        copy.wait()
    for s, done in blocks(-1, rows + 2):
        x = take(other, s + 1, SPAN)
        slope = slope_of(a0, s + 5 + done, BLOCK - done)
        keep(e0, split, s + 1 + done, wide_conv(band0[96 * done :, :], *x) * slope)

    own = slice(8, 8 + rows)
    cells = (rows + 2) * 32
    high, low = eh[0:cells, :], el[0:cells, :]
    wh, wl = band_out[0, :, :cells], band_out[1, :, :cells]
    y = (
        jnp.dot(wh, high, preferred_element_type=F32)
        + jnp.dot(wh, low, preferred_element_type=F32)
        + jnp.dot(wl, high, preferred_element_type=F32)
    )
    through = []
    for c in range(2):
        parts = [y[(2 * q + c) * rows : (2 * q + c + 1) * rows] for q in range(3)]
        through.append(turn(parts[0], 1, 1) + parts[1] + turn(parts[2], -1, 1))

    cross = []
    for k in range(2):
        flux = v[0] * adjoint[k]
        side = v[1][own] * adjoint[k][own]
        cross.append(
            ((turn(flux, -1, 0) - turn(flux, 1, 0)) * 0.5)[own]
            + (turn(side, -1, 1) - turn(side, 1, 1)) * 0.5
        )
    along_x = [((turn(f, -1, 0) - turn(f, 1, 0)) * 0.5)[own] for f in v]
    along_y = [(turn(f[own], -1, 1) - turn(f[own], 1, 1)) * 0.5 for f in v]
    direct = [
        adjoint[0][own] * along_x[0] + adjoint[1][own] * along_x[1],
        adjoint[0][own] * along_y[0] + adjoint[1][own] * along_y[1],
    ]
    for k in range(2):
        grad_velocity[k] = adjoint[k][own] - step_size * (direct[k] - cross[k]) + through[k]

    scale = factor[0, 0]
    middle1 = wide_terms(e2, 3, a1, 4, rows)
    middle0 = wide_terms(e1, 2, a0, 5, rows)

    outer = jnp.concatenate([sided(e3[c][own], 0) for c in range(2)], axis=0)
    lh, ll = halves(outer)
    ah, al = take(a2, 2, rows + 4)
    last = dot_nt(lh, ah) + dot_nt(lh, al) + dot_nt(ll, ah)
    last = last.reshape(6, rows, (rows + 4) * 32)
    group = lax.broadcasted_iota(jnp.int32, (rows, (rows + 4) * 32), 1) // 32
    line = lax.broadcasted_iota(jnp.int32, (rows, (rows + 4) * 32), 0)
    last = [
        eight_rows(
            lane_groups_summed(
                jnp.sum(jnp.where((group == line + p)[None], last, 0.0), axis=1)
            )
        )
        for p in range(3)
    ]

    inner = jnp.concatenate(
        [jnp.concatenate([turn(f, 1, 1), f, turn(f, -1, 1)], axis=0) for f in v], axis=0
    )
    lh, ll = halves(inner)
    eh0, el0 = high[32 : 32 + rows * 32], low[32 : 32 + rows * 32]
    begin = dot_nt(lh, eh0) + dot_nt(lh, el0) + dot_nt(ll, eh0)
    tall = rows + 16
    begin = begin.reshape(6, tall, rows * 32)
    group = lax.broadcasted_iota(jnp.int32, (tall, rows * 32), 1) // 32
    line = lax.broadcasted_iota(jnp.int32, (tall, rows * 32), 0)
    begin = [
        eight_rows(
            lane_groups_summed(
                jnp.sum(jnp.where((line == group + p + 7)[None], begin, 0.0), axis=1)
            )
        )
        for p in range(3)
    ]

    lane = lax.broadcasted_iota(jnp.int32, (1, 128), 1)
    ends = jnp.zeros((1, 128), F32)
    for c in range(2):
        end = jnp.sum(jnp.sum(e3[c][own], axis=0, keepdims=True), axis=1, keepdims=True)
        ends = ends + jnp.where(lane == 96 + c, end, 0.0)
    sums = [bias_line(e2, 3, rows), bias_line(e1, 2, rows), bias_line(e0, 1, rows), ends]
    sums = eight_rows(jnp.concatenate(sums, axis=0))
    kept = lax.broadcasted_iota(jnp.int32, (96, 128), 1) < 96
    rest = jnp.concatenate(last + begin + [sums, jnp.zeros((40, 128), F32)], axis=0)
    terms[0:96, :] = jnp.where(kept, middle1, rest) * scale
    terms[96:192, :] = jnp.where(kept, middle0, 0.0) * scale


def unpack_kernel(total, first, bias0, hidden, biases, last, ends):
    for p in range(3):
        for at, begin in enumerate((96, 0)):
            hidden[at, p] = total[begin : begin + 96, 32 * p : 32 * p + 32].reshape(3, 32, 32)
    rest = turn(total[0:56, :], 32, 1)[:, :32]
    for p in range(3):
        for ref, begin in ((last, 8 * p), (first, 24 + 8 * p)):
            for q in range(3):
                at = begin + q
                ref[p, q] = jnp.concatenate([rest[at : at + 1], rest[at + 3 : at + 4]], axis=0)
    biases[...] = jnp.concatenate([rest[49:50], rest[48:49]], axis=0)
    bias0[...] = rest[50:51]
    ends[...] = rest[51:52, :2]


def total_of(packed):
    lines, lanes = packed.shape
    local = (NEAR, CORE)
    part = packed.reshape(lax.axis_size(local), -1, lanes)
    part = lax.all_to_all(part, local, 0, 0, tiled=True).sum(axis=0)
    part = from_everyone(part, FAR).sum(axis=0)
    return from_everyone(part, local).reshape(lines, lanes)


def forward_taps(w):
    out, into = w.shape[2], w.shape[3]
    return jnp.transpose(w, (1, 2, 0, 3)).reshape(3 * out, 3 * into)


def backward_taps(w):
    out, into = w.shape[2], w.shape[3]
    return jnp.transpose(w[::-1, ::-1], (1, 3, 0, 2)).reshape(3 * into, 3 * out)


def narrow_taps(w):
    t = jnp.transpose(w, (2, 1, 3, 0))
    t = jnp.pad(t, ((0, 0), (0, 0), (0, 0), (0, 5))).reshape(w.shape[2], 48)
    return jnp.pad(t, ((0, 0), (0, 80)))


def out_taps_of(w):
    t = jnp.pad(w.reshape(3, 6, w.shape[3]), ((0, 0), (0, 2), (0, 0)))
    return jnp.concatenate([t] * 4, axis=2)


def flipped(w):
    return jnp.swapaxes(w[::-1, ::-1], 2, 3)


def shape_of(*dims, dtype=F32):
    return jax.ShapeDtypeStruct(dims, dtype)


def call(kernel, out_shape, scratch=(), room=63, **extra):
    return pl.pallas_call(
        kernel,
        out_shape=out_shape,
        scratch_shapes=list(scratch),
        compiler_params=pltpu.CompilerParams(vmem_limit_bytes=room * 1024 * 1024),
        **extra,
    )


def body(velocity, cotangent, w_first, b_first, w_hidden, b_hidden, w_last):
    rows, width = velocity.shape[1], velocity.shape[2]
    members = lax.axis_size(GX)
    cprev, clater = shifted(cotangent, GX, 1), shifted(cotangent, GX, -1)
    basis, sums, around = call(
        basis_kernel,
        (
            shape_of(ITERS, rows + 16, width),
            shape_of(members, 128),
            shape_of(2, rows + 16, width),
        ),
        room=16,
    )(cprev, cotangent, clater)
    gathered = lax.all_to_all(sums.reshape(members, 1, 128), GX, 0, 0, tiled=True)

    sums, w_first, b_first, w_hidden, b_hidden, w_last = lax.optimization_barrier(
        (sums, w_first, b_first, w_hidden, b_hidden, w_last)
    )
    sums, velocity = lax.optimization_barrier((sums, velocity))
    vprev, vlater = shifted(velocity, GX, 1), shifted(velocity, GX, -1)
    wide_pad = ((0, 0), (0, 256 - 96))
    wide = jnp.stack([jnp.pad(forward_taps(w_hidden[m]), wide_pad) for m in range(2)])
    wide_back = jnp.stack([jnp.pad(backward_taps(w_hidden[m]), wide_pad) for m in range(2)])
    narrow = narrow_taps(w_first)
    narrow_back = narrow_taps(flipped(w_last))
    out_taps = out_taps_of(flipped(w_first))
    biases = jnp.stack([b_first, b_hidden[0], b_hidden[1]])
    biases = jnp.broadcast_to(biases[:, :, None], (3, biases.shape[1], 128))

    heights = (rows + 10, rows + 8, rows + 6)
    held = [shape_of(h * 32, width, dtype=BF16) for h in heights for _ in range(2)]
    wide_band = shape_of(96 * BLOCK, 3 * SPAN * 32, dtype=BF16)
    narrow_band = shape_of(32 * BLOCK, 144, dtype=BF16)
    edge = -(-(rows + 2) * 32 // 128) * 128
    held += [narrow_band, wide_band, wide_band, shape_of(2, 6 * rows, edge, dtype=BF16)]
    a0h, a0l, a1h, a1l, a2h, a2l, band2, band1, band0, band_out = call(
        forward_kernel,
        tuple(held),
        [pltpu.VMEM(item.shape, item.dtype) for item in (narrow_band, wide_band, wide_band)],
    )(vprev, velocity, vlater, narrow, wide, biases, narrow_back, wide_back, out_taps)

    quick, unsafe = call(
        pressure_kernel,
        (shape_of(rows + 16, width), shape_of(1, 1, dtype=jnp.int32)),
        room=12,
        out_specs=(
            pl.BlockSpec(memory_space=pltpu.VMEM),
            pl.BlockSpec(memory_space=pltpu.SMEM),
        ),
    )(gathered.reshape(members, 128), basis)
    pressure = lax.cond(
        unsafe[0, 0] != 0,
        lambda c, _: stepwise_pressure(c),
        lambda c, q: q,
        around,
        quick,
    )

    factor = 1.0 / jnp.sqrt(jnp.float32(members * rows * width))
    whole = pl.BlockSpec(memory_space=pltpu.VMEM)
    outside = pl.BlockSpec(memory_space=pl.ANY)
    fetched = (band2, a2h, a2l, band1, a1h, a1l, band0, a0h, a0l, band_out)
    grad_velocity, terms = call(
        backward_kernel,
        (shape_of(2, rows, width), shape_of(192, 128)),
        [
            pltpu.VMEM(((rows + 6) * 32, width), F32),
            pltpu.VMEM(((rows + 4) * 32, width), F32),
            pltpu.VMEM(((rows + 2) * 32, width), F32),
            pltpu.VMEM(((rows + 6) * 32, width), BF16),
            pltpu.VMEM(((rows + 6) * 32, width), BF16),
            pltpu.VMEM(((rows + 4) * 32, width), BF16),
            pltpu.VMEM(((rows + 4) * 32, width), BF16),
        ]
        + [pltpu.VMEM(item.shape, item.dtype) for item in fetched]
        + [pltpu.SemaphoreType.DMA((len(fetched),))],
        in_specs=[pl.BlockSpec(memory_space=pltpu.SMEM)] + [whole] * 5 + [outside] * len(fetched),
    )(factor.reshape(1, 1), pressure, around, vprev, velocity, vlater, *fetched)
    total = total_of(terms)
    taps = w_first.shape[0]
    first, bias0, hidden, biases, last, ends = call(
        unpack_kernel,
        (
            shape_of(taps, taps, 2, 32),
            shape_of(1, 32),
            shape_of(2, taps, taps, 32, 32),
            shape_of(2, 32),
            shape_of(taps, taps, 2, 32),
            shape_of(1, 2),
        ),
    )(total)
    return (
        grad_velocity,
        jnp.swapaxes(first, 2, 3),
        bias0.reshape(-1),
        hidden,
        biases,
        last,
        ends.reshape(-1),
    )


def solution(mesh):
    cores, near = 2, 4
    far = mesh.shape["gx"] // (cores * near)
    finer = Mesh(mesh.devices.reshape(mesh.shape["groups"], far, near, cores), GROUPS_GX)
    placed = (P(None, GROUPS_GX, None), P(None, GROUPS_GX, None), P(), P(), P(), P(), P())
    return jax.shard_map(
        body,
        mesh=finer,
        in_specs=placed,
        out_specs=(
            P(None, GROUPS_GX, None),
            P("groups", None, None, None),
            P("groups"),
            P("groups", None, None, None, None),
            P("groups", None),
            P("groups", None, None, None),
            P("groups"),
        ),
        check_vma=False,
    )
```
